32 devices in a mesh: gz: 2 (over x), row: 4 (over y, core), col: 4 (over z).
Axes of the slice: x: 2, y: 2, z: 4, core: 2. Of those that a mesh axis runs over, the one named last changes fastest.
Arguments:
- sections: bfloat16 [4, 2048, 2048], P('gz', 'row', 'col'), may hold values from -6 to 6
- priors: int32 [2, 4, 8, 8], P(None, 'gz', 'row', 'col'), may hold values from -64 to 64
- row_order: int32 [8], replicated, may hold values from 0 to 7, each once
Outputs:
- mesh_flows: float32 [8, 64], P('row')
The draws below stay inside these ranges and needn't reach their ends.
Inputs may be any that keep to these rules, and one draw needn't show every extreme that they name: A permutation of the patch rows: mesh row m holds patch row row_order[m].
All inputs are finite; a program needn't handle non-finite values.
Results may differ from the reference program's by a relative error of at most 0.0003.
Values may be sent and summed in bfloat16 or wider, within the bound.
A program may use at most 64 MiB of HBM per device.

```python
import math
import jax
import jax.numpy as jnp
from jax import lax

PATCH = 512
STRIDE = 256
LAGS = 128
MAXOFF = 64
HALO = 256
SECTIONS = 4
HEIGHT = 2048
WIDTH = 2048
GRID_R = 8
GRID_C = 8


def shared_shifts(key):
    shift_key = jax.random.fold_in(key, 4242)
    reach = MAXOFF // 8
    starts = jax.random.randint(jax.random.fold_in(shift_key, 1), (2, SECTIONS), -reach, reach + 1)
    slopes = jax.random.randint(jax.random.fold_in(shift_key, 2), (2, SECTIONS), -reach, reach + 1)
    return (starts, slopes)


def moved_by(starts, slopes, coords, extent):
    return starts[:, None] + slopes[:, None] * coords[None, :] // extent


def draw_sections(key, part):
    starts, slopes = shared_shifts(key)
    rows_all = jnp.arange(HEIGHT, dtype=jnp.int32)
    cols_all = jnp.arange(WIDTH, dtype=jnp.int32)
    row_shift = moved_by(starts[0], slopes[0], rows_all, HEIGHT)
    col_shift = moved_by(starts[1], slopes[1], cols_all, WIDTH)
    margin = MAXOFF
    texture_key = jax.random.fold_in(key, 11)
    noise_key = jax.random.fold_in(key, 12)
    texture = jax.random.normal(texture_key, (HEIGHT + 2 * margin, WIDTH + 2 * margin), jnp.float32)
    noise = jax.random.normal(noise_key, (SECTIONS, HEIGHT, WIDTH), jnp.float32)
    signal_weight = 0.9
    noise_weight = 0.45
    level = 1.0
    row_index = rows_all[None, :] - row_shift + margin
    col_index = cols_all[None, :] - col_shift + margin

    def one_section(row_pick, col_pick):
        return jnp.take(jnp.take(texture, row_pick, axis=0), col_pick, axis=1)
    moved = jax.vmap(one_section)(row_index, col_index)
    result = level * (signal_weight * moved + noise_weight * noise)
    return jnp.clip(result, -6.0, 6.0).astype(jnp.bfloat16)


def draw_priors(key, part):
    starts, slopes = shared_shifts(key)
    center_gap = PATCH // 2 - HALO // 2
    row_centers = jnp.clip(jnp.arange(GRID_R, dtype=jnp.int32) * STRIDE + center_gap, 0, HEIGHT - 1)
    col_centers = jnp.clip(jnp.arange(GRID_C, dtype=jnp.int32) * STRIDE + center_gap, 0, WIDTH - 1)
    row_shift = moved_by(starts[0], slopes[0], row_centers, HEIGHT)
    col_shift = moved_by(starts[1], slopes[1], col_centers, WIDTH)
    row_lag = jnp.roll(row_shift, -1, axis=0) - row_shift
    col_lag = jnp.roll(col_shift, -1, axis=0) - col_shift
    slack = MAXOFF // 2
    jitter = jax.random.randint(jax.random.fold_in(key, 13), (2, SECTIONS, GRID_R, GRID_C), -slack, slack + 1)
    row_prior = row_lag[:, :, None] + jitter[0]
    col_prior = col_lag[:, None, :] + jitter[1]
    result = jnp.clip(jnp.stack([row_prior, col_prior], axis=0), -MAXOFF, MAXOFF)
    result = result.at[0, 0, 0, 0].set(MAXOFF)
    result = result.at[0, SECTIONS - 1, 0, 0].set(-MAXOFF)
    result = result.at[1, 0, 0, 0].set(-MAXOFF)
    result = result.at[1, SECTIONS - 1, 0, 0].set(MAXOFF)
    return result.astype(jnp.int32)


def setup_inputs(seed: int = 0) -> dict:
    splits = jax.random.split(jax.random.key(seed), 4)
    sections = draw_sections(jax.random.fold_in(splits[3], 71), 0)
    priors = draw_priors(jax.random.fold_in(splits[3], 71), 0)
    row_order = jax.random.permutation(splits[2], GRID_R).astype(jnp.int32)
    return dict(sections=sections, priors=priors, row_order=row_order)


def dft_tables(length):
    frequencies = jnp.arange(length, dtype=jnp.int32)
    angles = jnp.mod(frequencies[:, None] * frequencies[None, :], length).astype(jnp.float32) * (2.0 * math.pi / length)
    cosine = jnp.cos(angles)
    sine_part = jnp.sin(angles)
    minus_table = jnp.concatenate([cosine, -sine_part], axis=1).astype(jnp.bfloat16)
    plus_table = jnp.concatenate([cosine, sine_part], axis=1).astype(jnp.bfloat16)
    return minus_table, plus_table


def spectra_of(patches, minus_table, plus_table):
    length = patches.shape[-1]
    row_pass = jnp.einsum('nxy,yk->nxk', patches.astype(jnp.float32), minus_table.astype(jnp.float32)).astype(jnp.bfloat16)
    real_rows = row_pass[:, :, :length]
    imag_rows = row_pass[:, :, length:]
    upper_stack = jnp.concatenate([real_rows, imag_rows], axis=1).astype(jnp.float32)
    lower_stack = jnp.concatenate([imag_rows, real_rows], axis=1).astype(jnp.float32)
    spec_real = jnp.einsum('kx,nxm->nkm', plus_table.astype(jnp.float32), upper_stack) / length
    spec_imag = jnp.einsum('kx,nxm->nkm', minus_table.astype(jnp.float32), lower_stack) / length
    return jnp.stack([spec_real, spec_imag], axis=1).astype(jnp.bfloat16)


def lag_angles(offsets, length):
    frequencies = jnp.arange(length, dtype=jnp.int32)
    shifts = offsets[:, None] + jnp.arange(LAGS, dtype=jnp.int32)[None, :] - LAGS // 2
    angles = jnp.mod(shifts[:, :, None] * frequencies[None, None, :], length).astype(jnp.float32) * (2.0 * math.pi / length)
    return jnp.cos(angles), jnp.sin(angles)


def flows_of(first_spec, second_spec, offsets):
    length = first_spec.shape[-1]
    first_real = first_spec[:, 0].astype(jnp.float32)
    first_imag = first_spec[:, 1].astype(jnp.float32)
    second_real = second_spec[:, 0].astype(jnp.float32)
    second_imag = second_spec[:, 1].astype(jnp.float32)
    prod_real = (first_real * second_real + first_imag * second_imag).astype(jnp.bfloat16)
    prod_imag = (first_real * second_imag - first_imag * second_real).astype(jnp.bfloat16)
    row_cosine, row_sine = lag_angles(offsets[0], length)
    column_cosine, column_sine = lag_angles(offsets[1], length)
    products = jnp.concatenate([prod_real, prod_imag], axis=2).astype(jnp.float32)
    column_real = jnp.concatenate([column_cosine, -column_sine], axis=2).astype(jnp.bfloat16).astype(jnp.float32)
    column_imag = jnp.concatenate([column_sine, column_cosine], axis=2).astype(jnp.bfloat16).astype(jnp.float32)
    half_real = jnp.einsum('nkl,nul->nku', products, column_real).astype(jnp.bfloat16)
    half_imag = jnp.einsum('nkl,nul->nku', products, column_imag).astype(jnp.bfloat16)
    row_table = jnp.concatenate([row_cosine, -row_sine], axis=2).astype(jnp.bfloat16).astype(jnp.float32)
    stacked = jnp.concatenate([half_real, half_imag], axis=1).astype(jnp.float32)
    surface = jnp.einsum('ntk,nku->ntu', row_table, stacked) / length
    weights = surface * surface
    displacement = (jnp.arange(LAGS, dtype=jnp.int32) - LAGS // 2).astype(jnp.float32)
    weight_sum = 1.0 + jnp.sum(weights, axis=(1, 2))
    row_shift = jnp.sum(weights * displacement[None, :, None], axis=(1, 2)) / weight_sum
    column_shift = jnp.sum(weights * displacement[None, None, :], axis=(1, 2)) / weight_sum
    return jnp.stack([offsets[0].astype(jnp.float32) + row_shift, offsets[1].astype(jnp.float32) + column_shift], axis=0)


def reference(sections, priors, row_order):
    minus_table, plus_table = dft_tables(PATCH)
    margin = HALO // 2
    padded = jnp.pad(sections, ((0, 0), (margin, HALO - margin), (margin, HALO - margin)))
    place_count = GRID_R * GRID_C
    offsets_all = jnp.transpose(priors, (2, 3, 0, 1)).reshape(place_count, 2, SECTIONS)
    positions = jnp.arange(place_count, dtype=jnp.int32)

    def one_place(inputs):
        position, offsets = inputs
        top_edge = (position // GRID_C) * STRIDE
        left_edge = (position % GRID_C) * STRIDE
        window = lax.dynamic_slice(padded, (jnp.int32(0), top_edge.astype(jnp.int32), left_edge.astype(jnp.int32)), (SECTIONS, PATCH, PATCH))
        spectra = spectra_of(window, minus_table, plus_table)
        following = jnp.concatenate([spectra[1:], spectra[:1]], axis=0)
        return flows_of(spectra, following, offsets)

    all_flows = lax.map(one_place, (positions, offsets_all))
    flow_table = jnp.transpose(all_flows.reshape(GRID_R, GRID_C, 2, SECTIONS), (2, 3, 0, 1))
    picked = flow_table[:, :, row_order, :]
    return jnp.transpose(picked, (2, 0, 1, 3)).reshape(GRID_R, 2 * SECTIONS * GRID_C)
```

```python
import math

import jax
import jax.numpy as jnp
import numpy as np
from jax import lax
from jax.experimental import pallas as pl
from jax.experimental.pallas import tpu as pltpu
from jax.sharding import PartitionSpec as P

PATCH = 512
STRIDE = 256
LAGS = 128
HALO = 256
HALF = PATCH // 2
QUARTER = PATCH // 4
KROWS = HALF + 16


def angle_of(products):
    return (products % PATCH) * (2.0 * math.pi / PATCH)


def dft_table():
    k = np.arange(HALF)[:, None]
    x = np.arange(PATCH)[None, :]
    table = np.zeros((2 * KROWS, PATCH))
    table[:HALF] = np.cos(angle_of(k * x))
    table[HALF] = np.cos(angle_of(HALF * x[0]))
    table[KROWS : KROWS + HALF] = -np.sin(angle_of(k * x))
    return table


def split_tables():
    y = np.arange(QUARTER)[:, None]
    blocks = []
    for g in range(4):
        l = 4 * np.arange(QUARTER)[None, :] + g
        c, s = np.cos(angle_of(y * l)), np.sin(angle_of(y * l))
        blocks.append(np.block([[c, -s], [s, c]]))
    return np.stack(blocks)


def lag_tables():
    lag = np.arange(2 * LAGS)[:, None] - LAGS
    l = np.concatenate([4 * np.arange(QUARTER) + g for g in range(4)])[None, :]
    k = np.arange(KROWS)[None, :]
    weight = np.where(k == 0, 1.0, np.where(k < HALF, 2.0, np.where(k == HALF, 1.0, 0.0)))
    col = (np.cos(angle_of(lag * l)), np.sin(angle_of(lag * l)))
    row_cos = np.cos(angle_of(lag * k)) * weight
    row_sin = -np.sin(angle_of(lag * k)) * weight
    row = np.concatenate([row_cos, row_sin], axis=1)
    return col[0], col[1], row


def bf16_const(value):
    return value.astype(np.float32).astype(jnp.bfloat16)


def f32_const(value):
    return bf16_const(value).astype(np.float32)


def first_pass(ext, section, i, dft_ref, pq_ref, slot, outer):
    rows = pl.ds(pl.multiple_of(i * STRIDE, STRIDE), PATCH)
    edge, far = HALO // 2, ext.shape[2] - HALO // 2
    if not outer:
        pq_ref[slot, :, edge:far] = jnp.dot(
            dft_ref[...], ext[section, rows, edge:far], preferred_element_type=jnp.float32
        )
        return
    window = jnp.concatenate([ext[section, rows, :edge], ext[section, rows, far:]], axis=1)
    both = jnp.dot(dft_ref[...], window, preferred_element_type=jnp.float32)
    pq_ref[slot, :, :edge] = both[:, :edge]
    pq_ref[slot, :, far:] = both[:, edge:]


def spectrum_pair(wg_ref, spec_ref, pq_ref, slot, base):
    for j in range(2):
        p, q = [], []
        for t in range(4):
            lanes = slice(j * STRIDE + t * QUARTER, j * STRIDE + (t + 1) * QUARTER)
            p.append(pq_ref[slot, :KROWS, lanes])
            q.append(pq_ref[slot, KROWS:, lanes])
        ps, pd, qs, qd = p[0] + p[2], p[0] - p[2], q[0] + q[2], q[0] - q[2]
        pt, pu, qt, qu = p[1] + p[3], p[1] - p[3], q[1] + q[3], q[1] - q[3]
        groups = ((ps + pt, qs + qt), (pd + qu, qd - pu), (ps - pt, qs - qt), (pd - qu, qd + pu))
        for g, (real, imag) in enumerate(groups):
            left = jnp.concatenate([real.astype(jnp.bfloat16), imag.astype(jnp.bfloat16)], axis=1)
            out = jnp.dot(left, wg_ref[g], preferred_element_type=jnp.float32).astype(jnp.bfloat16)
            lo = g * QUARTER
            spec_ref[base + j, :, lo : lo + QUARTER] = out[:, :QUARTER]
            spec_ref[base + j, :, PATCH + lo : PATCH + lo + QUARTER] = out[:, QUARTER:]


def lag_rows(table, prior):
    tiles = [
        table[t, pl.ds(prior + LAGS // 2, LAGS), :].astype(jnp.bfloat16)
        for t in range(table.shape[0])
    ]
    return jnp.concatenate(tiles, axis=1)


def lane_tiles(table):
    width = -(-table.shape[1] // LAGS) * LAGS
    table = np.pad(table, ((0, 0), (0, width - table.shape[1])))
    return np.stack(np.split(table, width // LAGS, axis=1))


def pair_flow(first, second, p, q, spec_ref, colc_ref, cols_ref, row_ref):
    f32 = jnp.float32
    ar = spec_ref[first, :, :PATCH].astype(f32)
    ai = spec_ref[first, :, PATCH:].astype(f32)
    br = spec_ref[second, :, :PATCH].astype(f32)
    bi = spec_ref[second, :, PATCH:].astype(f32)
    cr = (ar * br + ai * bi).astype(jnp.bfloat16)
    ci = (ar * bi - ai * br).astype(jnp.bfloat16)
    ec = lag_rows(colc_ref, q)
    es = lag_rows(cols_ref, q)
    left = jnp.concatenate([cr, ci], axis=1)
    right = jnp.concatenate(
        [jnp.concatenate([ec, -es], axis=1), jnp.concatenate([es, ec], axis=1)], axis=0
    )
    half = lax.dot_general(
        left, right, (((1,), (1,)), ((), ())), preferred_element_type=f32
    ).astype(jnp.bfloat16)
    stacked = jnp.concatenate([half[:, :LAGS], half[:, LAGS:]], axis=0)
    rows = lag_rows(row_ref, p)[:, : 2 * KROWS]
    surface = jnp.dot(rows, stacked, preferred_element_type=f32) * (1.0 / PATCH**3)
    w = surface * surface
    da = (lax.broadcasted_iota(jnp.int32, (LAGS, LAGS), 0) - LAGS // 2).astype(f32)
    db = (lax.broadcasted_iota(jnp.int32, (1, LAGS), 1) - LAGS // 2).astype(f32)
    col_w = jnp.sum(w, axis=0, keepdims=True)
    total = 1.0 + jnp.sum(col_w, axis=1, keepdims=True)
    row_m = jnp.sum(jnp.sum(w * da, axis=0, keepdims=True), axis=1, keepdims=True)
    col_m = jnp.sum(col_w * db, axis=1, keepdims=True)
    return p.astype(f32) + row_m / total, q.astype(f32) + col_m / total


def make_kernel(sizes, rows_each):
    size_gz, size_row, size_col = sizes
    count = size_gz * size_row * size_col
    side = 2 * STRIDE
    margin = HALO // 2
    far = side - margin
    inner = far - margin
    mesh_id = pl.DeviceIdType.MESH
    cross = ((-1, 0), (1, 0), (0, -1), (0, 1))
    diagonal = ((-1, -1), (-1, 1), (1, -1), (1, 1))
    partners = sorted({1 % size_gz, size_gz - 1} - {0})
    reaches = doubling(sizes)
    rounds = len(reaches) + 2
    span = {-1: (0, margin), 0: (0, side), 1: (far, margin)}
    halo = {-1: (-margin, margin), 0: (0, side), 1: (side, margin)}
    chunks = (
        (0, margin, 0, margin), (0, margin, far, margin),
        (far, margin, 0, margin), (far, margin, far, margin),
        (margin, inner, 0, margin), (margin, inner, far, margin),
        (0, margin, margin, inner), (far, margin, margin, inner),
        (margin, inner, margin, inner),
    )
    copies = halo_copies(span, halo, margin, inner, cross, diagonal)

    def pick(section, *kinds):
        return [n for n, c in enumerate(copies) if c[0] == section and c[1] in kinds]

    def kernel(
        pri_hbm, order_hbm, sec_hbm, dft_hbm, wg_hbm, colc_hbm, cols_hbm, row_hbm, out_ref,
        ext, dft_ref, wg_ref, colc_ref, cols_ref, row_ref, spec_ref, pq_ref, mine_ref, all_ref,
        load_sem, halo_send, halo_recv, chunk_send, chunk_recv, flow_send, flow_recv, flood, pri_ref,
        order_ref,
    ):
        gz, row, col = lax.axis_index("gz"), lax.axis_index("row"), lax.axis_index("col")
        flat = (gz * size_row + row) * size_col + col

        def device(number):
            return (
                number // (size_row * size_col),
                (number // size_col) % size_row,
                number % size_col,
            )

        def exists(step):
            a, b = step
            ok = None
            for delta, place, size in ((a, row, size_row), (b, col, size_col)):
                if delta:
                    this = place > 0 if delta < 0 else place < size - 1
                    ok = this if ok is None else jnp.logical_and(ok, this)
            return ok

        near = len(partners)
        for step in cross:
            near = near + exists(step).astype(jnp.int32)

        def greet():
            barrier = pltpu.get_barrier_semaphore()
            for other in partners:
                pl.semaphore_signal(
                    barrier, 1, device_id=((gz + other) % size_gz, row, col),
                    device_id_type=mesh_id,
                )
            for step in cross:
                @pl.when(exists(step))
                def _(step=step):
                    pl.semaphore_signal(
                        barrier, 1, device_id=(gz, row + step[0], col + step[1]),
                        device_id_type=mesh_id,
                    )


        greet()
        loads = [
            pltpu.make_async_copy(
                sec_hbm.at[n], ext.at[n, margin : margin + side, margin : margin + side],
                load_sem.at[n],
            )
            for n in range(2)
        ]
        tables = (
            (dft_hbm, dft_ref), (wg_hbm, wg_ref), (colc_hbm, colc_ref), (cols_hbm, cols_ref),
            (row_hbm, row_ref), (pri_hbm, pri_ref), (order_hbm, order_ref),
        )
        for n, (source, target) in enumerate(tables):
            loads.append(pltpu.make_async_copy(source, target, load_sem.at[n + 2]))
        for copy in loads:
            copy.start()

        def place(section, r0, rn, c0, cn):
            return ext.at[
                section, margin + r0 : margin + r0 + rn, margin + c0 : margin + c0 + cn
            ]

        def landing(n):
            section, _, (a, b), _, (r0, rn, c0, cn) = copies[n]
            return place(section, r0 - a * side, rn, c0 - b * side, cn)

        def halo_copy(n):
            section, _, (a, b), _, box = copies[n]
            return pltpu.make_async_remote_copy(
                src_ref=place(section, *box), dst_ref=landing(n),
                send_sem=halo_send.at[n], recv_sem=halo_recv.at[n],
                device_id=(gz, row + a, col + b), device_id_type=mesh_id,
            )

        def guard(n, sign):
            (a, b), side_col = copies[n][2], copies[n][3]
            return exists((sign * a, side_col if side_col else sign * b))

        def send(numbers):
            for n in numbers:
                @pl.when(guard(n, 1))
                def _(n=n):
                    halo_copy(n).start()

        def arrive(numbers):
            for n in numbers:
                @pl.when(guard(n, -1))
                def _(n=n):
                    ref = landing(n)
                    pltpu.make_async_copy(ref, ref, halo_recv.at[n]).wait()

        def chunk_copy(n):
            return pltpu.make_async_remote_copy(
                src_ref=place(0, *chunks[n]), dst_ref=place(2, *chunks[n]),
                send_sem=chunk_send.at[n], recv_sem=chunk_recv.at[n],
                device_id=((gz + size_gz - 1) % size_gz, row, col), device_id_type=mesh_id,
            )

        def took(low, high):
            for n in range(low, high):
                chunk_copy(n).wait_recv()

        def rung(n):
            if n < len(reaches):
                k = reaches[n]
                lines = []
                for way in (-k, k):
                    for axis, at, size in ((1, row, size_row), (2, col, size_col)):
                        ok = at + way >= 0 if way < 0 else at + way < size
                        lines.append((ok, (gz, row + way, col) if axis == 1 else (gz, row, col + way)))
                return lines
            if n == len(reaches):
                return [(None, (gz, row, (col + j) % size_col)) for j in range(1, size_col)]
            return [(None, ((gz + j) % size_gz, row, col)) for j in range(1, size_gz)]

        def climb(n):
            for ok, target in rung(n):
                def tell(target=target):
                    pl.semaphore_signal(
                        flood.at[n], 1, device_id=target, device_id_type=mesh_id
                    )
                if ok is None:
                    tell()
                else:
                    pl.when(ok)(tell)

        def heard(n):
            total = 0
            for ok, _ in rung(n):
                total = total + (1 if ok is None else ok.astype(jnp.int32))
            return total

        done = [0]

        def spread(upto):
            for n in range(done[0], min(upto, rounds)):
                pl.semaphore_wait(flood.at[n], heard(n))
                if n + 1 < rounds:
                    climb(n + 1)
            done[0] = max(done[0], min(upto, rounds))

        def middle(n, carry):
            first_pass(ext, n // 2, n % 2, dft_ref, pq_ref, n % 4, False)
            return carry

        def spectra(n, carry):
            first_pass(ext, n // 2, n % 2, dft_ref, pq_ref, n % 4, True)
            spectrum_pair(wg_ref, spec_ref, pq_ref, n % 4, n * 2)
            return carry

        for step in cross + diagonal:
            @pl.when(jnp.logical_not(exists(step)))
            def _(step=step):
                (r0, rn), (c0, cn) = halo[step[0]], halo[step[1]]
                ext[:, margin + r0 : margin + r0 + rn, margin + c0 : margin + c0 + cn] = (
                    jnp.zeros((3, rn, cn), ext.dtype)
                )

        mine_ref[...] = jnp.zeros_like(mine_ref)
        pl.semaphore_wait(pltpu.get_barrier_semaphore(), near)
        loads[0].wait()
        for n in range(len(chunks)):
            chunk_copy(n).start()
        send(pick(0, "row", "col"))
        loads[1].wait()
        send(pick(1, "row", "col"))
        climb(0)
        for copy in loads[2:]:
            copy.wait()

        lane = lax.broadcasted_iota(jnp.int32, (1, LAGS), 1)
        sections, columns = 2 * size_gz, 2 * size_col

        def prior(part, n):
            return pri_ref[part, n // 4, (n // 2) % 2, n % 2]

        def pairs_static(low, high):
            values = []
            for n in range(low, high):
                a, b = pair_flow(
                    n, n + 4, prior(0, n), prior(1, n), spec_ref, colc_ref, cols_ref, row_ref
                )
                at = (2 * gz + n // 4) * columns + 2 * col + n % 2
                values.append(
                    jnp.where(lane == at, a, 0.0)
                    + jnp.where(lane == at + sections * columns, b, 0.0)
                )
            mine_ref[0] = mine_ref[0] + values[0] + values[1]
            mine_ref[1] = mine_ref[1] + values[2] + values[3]

        arrive(pick(0, "row"))
        lax.fori_loop(0, 2, middle, 0, unroll=2)
        spread(1)
        took(0, 4)
        send(pick(2, "diagonal", "corner"))
        arrive(pick(0, "col"))
        send(pick(0, "turn"))
        arrive(pick(1, "row"))
        lax.fori_loop(2, 4, middle, 0, unroll=2)
        spread(2)
        took(4, 5)
        send(pick(2, "left"))
        arrive(pick(1, "col"))
        send(pick(1, "turn"))
        took(5, 6)
        send(pick(2, "right"))
        arrive(pick(0, "turn"))
        lax.fori_loop(0, 2, spectra, 0, unroll=2)
        spread(3)
        took(6, 7)
        send(pick(2, "up"))
        took(7, 8)
        send(pick(2, "down"))
        arrive(pick(1, "turn"))
        lax.fori_loop(2, 4, spectra, 0, unroll=2)
        pairs_static(0, 4)
        took(8, 9)
        arrive(pick(2, "up", "down", "corner"))
        lax.fori_loop(4, 6, middle, 0, unroll=2)
        arrive(pick(2, "left", "right", "diagonal"))
        lax.fori_loop(4, 6, spectra, 0, unroll=2)
        pairs_static(4, 8)
        spread(rounds)

        total_rows = 2 * size_row
        slot = gz * size_col + col
        spot = slot * total_rows + 2 * row

        rows_on = [(row + n) % size_row for n in range(size_row)]
        cols_on = [(col + n) % size_col for n in range(size_col)]
        for a in range(size_gz):
            plane = (gz + a) % size_gz
            for b in range(size_row):
                for c in range(size_col):
                    if a + b + c:
                        pltpu.make_async_remote_copy(
                            src_ref=mine_ref, dst_ref=all_ref.at[pl.ds(spot, 2)],
                            send_sem=flow_send, recv_sem=flow_recv,
                            device_id=(plane, rows_on[b], cols_on[c]), device_id_type=mesh_id,
                        ).start()
        all_ref[spot] = mine_ref[0]
        all_ref[spot + 1] = mine_ref[1]
        for n in range(len(chunks)):
            chunk_copy(n).wait_send()
        for n in range(len(copies)):
            @pl.when(guard(n, 1))
            def _(n=n):
                halo_copy(n).wait_send()
        got = all_ref.at[pl.ds(0, 2 * (count - 1))]
        pltpu.make_async_copy(got, got, flow_recv).wait()
        for m in range(rows_each):
            wanted = order_ref[row * rows_each + m]
            value = all_ref[wanted]
            for other in range(1, size_gz * size_col):
                value = value + all_ref[other * total_rows + wanted]
            out_ref[m : m + 1, :] = value[:, : out_ref.shape[1]]
        pltpu.make_async_copy(got, got, flow_send).wait()

    return kernel


def doubling(sizes):
    reaches = [1]
    while 2 * reaches[-1] < max(sizes[1:]):
        reaches.append(2 * reaches[-1])
    return reaches


def halo_copies(span, halo, margin, inner, cross, diagonal):
    copies = []
    for section in range(2):
        for step in cross:
            kind = "row" if step[0] else "col"
            copies.append((section, kind, step, 0, span[step[0]] + span[step[1]]))
        for a, b in diagonal:
            copies.append((section, "turn", (a, 0), b, span[a] + halo[b]))
    for a, b in diagonal:
        copies.append((2, "diagonal", (a, b), 0, span[a] + span[b]))
    for a, b in diagonal:
        copies.append((2, "corner", (a, 0), 0, span[a] + span[b]))
    for b in (-1, 1):
        copies.append((2, "left" if b < 0 else "right", (0, b), 0, span[0] + span[b]))
    for a in (-1, 1):
        copies.append((2, "up" if a < 0 else "down", (a, 0), 0, span[a] + (margin, inner)))
    return copies


def body(sections, priors, row_order):
    sizes = tuple(lax.axis_size(name) for name in ("gz", "row", "col"))
    count = math.prod(sizes)
    rows_each = row_order.shape[0] // sizes[1]
    width = 2 * 2 * sizes[0] * 2 * sizes[2]
    colc, cols, row = lag_tables()
    tables = (
        bf16_const(dft_table()),
        bf16_const(split_tables()),
        f32_const(lane_tiles(colc)),
        f32_const(lane_tiles(cols)),
        f32_const(lane_tiles(row)),
    )
    hbm = pl.BlockSpec(memory_space=pl.ANY)
    dma = pltpu.SemaphoreType.DMA
    wide = 2 * STRIDE + HALO
    flows = pl.pallas_call(
        make_kernel(sizes, rows_each),
        out_shape=jax.ShapeDtypeStruct((rows_each, width), jnp.float32),
        in_specs=[hbm] * 8,
        out_specs=pl.BlockSpec(memory_space=pltpu.VMEM),
        scratch_shapes=[
            pltpu.VMEM((3, wide, wide), jnp.bfloat16),
            *[pltpu.VMEM(t.shape, t.dtype) for t in tables],
            pltpu.VMEM((12, KROWS, 2 * PATCH), jnp.bfloat16),
            pltpu.VMEM((4, 2 * KROWS, wide), jnp.float32),
            pltpu.VMEM((2, 1, LAGS), jnp.float32),
            pltpu.VMEM((2 * count, 1, LAGS), jnp.float32),
            dma((9,)), dma((28,)), dma((28,)), dma((9,)), dma((9,)), dma(()), dma(()),
            pltpu.SemaphoreType.REGULAR((len(doubling(sizes)) + 2,)),
            pltpu.SMEM(priors.shape, priors.dtype), pltpu.SMEM(row_order.shape, row_order.dtype),
        ],
        compiler_params=pltpu.CompilerParams(
            vmem_limit_bytes=67043328, collective_id=0, has_side_effects=True
        ),
    )(priors, row_order, sections, *tables)
    return flows


def solution(mesh):
    placed = (P("gz", "row", "col"), P(None, "gz", "row", "col"), P())
    return jax.shard_map(
        body, mesh=mesh, in_specs=placed, out_specs=P("row", None), check_vma=False
    )
```

```python
import math

import jax
import jax.numpy as jnp
import numpy as np
from jax import lax
from jax.experimental import pallas as pl
from jax.experimental.pallas import tpu as pltpu
from jax.sharding import PartitionSpec as P

PATCH = 512
STRIDE = 256
LAGS = 128
MAXOFF = 64
HALO = 256
HALF = PATCH // 2
QUARTER = PATCH // 4
KROWS = HALF + 16


def angle_of(products):
    return (products % PATCH) * (2.0 * math.pi / PATCH)


def dft_table():
    k = np.arange(HALF)[:, None]
    x = np.arange(PATCH)[None, :]
    table = np.zeros((2 * KROWS, PATCH))
    table[:HALF] = np.cos(angle_of(k * x))
    table[HALF] = np.cos(angle_of(HALF * x[0]))
    table[KROWS : KROWS + HALF] = -np.sin(angle_of(k * x))
    return table


def split_tables():
    y = np.arange(QUARTER)[:, None]
    blocks = []
    for g in range(4):
        l = 4 * np.arange(QUARTER)[None, :] + g
        c, s = np.cos(angle_of(y * l)), np.sin(angle_of(y * l))
        blocks.append(np.block([[c, -s], [s, c]]))
    return np.stack(blocks)


def lag_table():
    lag = np.arange(2 * LAGS)[:, None] - LAGS
    k = np.arange(KROWS)[None, :]
    weight = np.where(k == 0, 1.0, np.where(k < HALF, 2.0, np.where(k == HALF, 1.0, 0.0)))
    row_cos = np.cos(angle_of(lag * k)) * weight
    row_sin = -np.sin(angle_of(lag * k)) * weight
    return np.concatenate([row_cos, row_sin], axis=1)


def column_tables():
    lag = np.arange(LAGS)[None, :] - LAGS // 2
    shift = np.arange(-MAXOFF, MAXOFF + 1)[:, None]
    matrix, phase = [], []
    for g in range(4):
        l = 4 * np.arange(QUARTER) + g
        c, s = np.cos(angle_of(l[:, None] * lag)), np.sin(angle_of(l[:, None] * lag))
        matrix.append(np.block([[c, s], [-s, c]]))
        phase += [np.cos(angle_of(shift * l)), np.sin(angle_of(shift * l))]
    return np.concatenate(matrix), np.concatenate(phase, axis=1)


def bf16_const(value):
    return value.astype(np.float32).astype(jnp.bfloat16)


def f32_const(value):
    return bf16_const(value).astype(np.float32)


def first_pass(ext, section, dft_ref, pq_ref, slot, spans):
    boxes = [(i, low, high) for i in range(2) for low, high in spans]
    window = [ext[section, i * STRIDE : i * STRIDE + PATCH, low:high] for i, low, high in boxes]
    both = jnp.dot(
        dft_ref[...], jnp.concatenate(window, axis=1), preferred_element_type=jnp.float32
    )
    at = 0
    for i, low, high in boxes:
        pq_ref[slot + i, :, low:high] = both[:, at : at + high - low]
        at += high - low


def spectrum(wg_ref, pq_ref, slot, j):
    p, q = [], []
    for t in range(4):
        lanes = slice(j * STRIDE + t * QUARTER, j * STRIDE + (t + 1) * QUARTER)
        p.append(pq_ref[slot, :KROWS, lanes])
        q.append(pq_ref[slot, KROWS:, lanes])
    ps, pd, qs, qd = p[0] + p[2], p[0] - p[2], q[0] + q[2], q[0] - q[2]
    pt, pu, qt, qu = p[1] + p[3], p[1] - p[3], q[1] + q[3], q[1] - q[3]
    groups = ((ps + pt, qs + qt), (pd + qu, qd - pu), (ps - pt, qs - qt), (pd - qu, qd + pu))
    for g, (real, imag) in enumerate(groups):
        left = jnp.concatenate([real.astype(jnp.bfloat16), imag.astype(jnp.bfloat16)], axis=1)
        out = jnp.dot(left, wg_ref[g], preferred_element_type=jnp.float32)
        yield g, out[:, :QUARTER], out[:, QUARTER:]


def spectrum_work(wg_ref, pq_ref, slot, j, turn_ref, at, cross_ref, phase):
    for g, re, im in spectrum(wg_ref, pq_ref, slot, j):
        low, mid, high = 2 * g * QUARTER, (2 * g + 1) * QUARTER, (2 * g + 2) * QUARTER
        if cross_ref is not None:
            ar, ai = turn_ref[at, :, low:mid], turn_ref[at, :, mid:high]
            cross_ref[at, :, low:mid] = (ar * re + ai * im).astype(jnp.bfloat16)
            cross_ref[at, :, mid:high] = (ar * im - ai * re).astype(jnp.bfloat16)
        if phase is not None:
            c, s = phase[:, low:mid], phase[:, mid:high]
            turn_ref[at, :, low:mid] = re * c + im * s
            turn_ref[at, :, mid:high] = im * c - re * s
        yield


def lag_rows(table, prior):
    tiles = [
        table[t, pl.ds(prior + LAGS // 2, LAGS), :].astype(jnp.bfloat16)
        for t in range(table.shape[0])
    ]
    return jnp.concatenate(tiles, axis=1)


def lane_tiles(table):
    width = -(-table.shape[1] // LAGS) * LAGS
    table = np.pad(table, ((0, 0), (0, width - table.shape[1])))
    return np.stack(np.split(table, width // LAGS, axis=1))


def half_work(cross_ref, n, e_ref, halves):
    total = None
    for g in range(4):
        part = slice(2 * g * QUARTER, 2 * (g + 1) * QUARTER)
        piece = jnp.dot(cross_ref[n, :, part], e_ref[part], preferred_element_type=jnp.float32)
        total = piece if total is None else total + piece
        if g == 3:
            halves[n] = total.astype(jnp.bfloat16)
        yield


def surface_of(half, rows):
    stacked = jnp.concatenate([half[:, :LAGS], half[:, LAGS:]], axis=0)
    return jnp.dot(rows, stacked, preferred_element_type=jnp.float32) * (1.0 / PATCH**3)


def centroid(surface, p, q):
    f32 = jnp.float32
    w = surface * surface
    da = (lax.broadcasted_iota(jnp.int32, (LAGS, LAGS), 0) - LAGS // 2).astype(f32)
    db = (lax.broadcasted_iota(jnp.int32, (1, LAGS), 1) - LAGS // 2).astype(f32)
    col_w = jnp.sum(w, axis=0, keepdims=True)
    total = 1.0 + jnp.sum(col_w, axis=1, keepdims=True)
    row_m = jnp.sum(jnp.sum(w * da, axis=0, keepdims=True), axis=1, keepdims=True)
    col_m = jnp.sum(col_w * db, axis=1, keepdims=True)
    return p.astype(f32) + row_m / total, q.astype(f32) + col_m / total


def interleave(*works):
    for _ in zip(*works):
        pass


def make_kernel(sizes, rows_each):
    size_gz, size_row, size_col = sizes
    count = size_gz * size_row * size_col
    side = 2 * STRIDE
    margin = HALO // 2
    far = side - margin
    inner = far - margin
    mesh_id = pl.DeviceIdType.MESH
    cross = ((-1, 0), (1, 0), (0, -1), (0, 1))
    diagonal = ((-1, -1), (-1, 1), (1, -1), (1, 1))
    partners = sorted({1 % size_gz, size_gz - 1} - {0})
    reaches = doubling(sizes)
    rounds = len(reaches) + 2
    span = {-1: (0, margin), 0: (0, side), 1: (far, margin)}
    halo = {-1: (-margin, margin), 0: (0, side), 1: (side, margin)}
    chunks = (
        (0, margin, 0, margin), (0, margin, far, margin),
        (far, margin, 0, margin), (far, margin, far, margin),
        (margin, inner, 0, margin), (margin, inner, far, margin),
        (0, margin, margin, inner), (far, margin, margin, inner),
        (margin, inner, margin, inner),
    )
    copies = halo_copies(span, halo, margin, inner, cross, diagonal)

    def pick(section, *kinds):
        return [n for n, c in enumerate(copies) if c[0] == section and c[1] in kinds]

    def kernel(
        pri_hbm, order_hbm, sec_hbm, dft_hbm, wg_hbm, e_hbm, phase_hbm, row_hbm, out_ref,
        ext, dft_ref, wg_ref, e_ref, phase_ref, row_ref, turn_ref, cross_ref, lags_ref, pq_ref,
        mine_ref, all_ref,
        load_sem, halo_send, halo_recv, chunk_send, chunk_recv, flow_send, flow_recv, flood, pri_ref,
        order_ref,
    ):
        gz, row, col = lax.axis_index("gz"), lax.axis_index("row"), lax.axis_index("col")
        flat = (gz * size_row + row) * size_col + col

        def device(number):
            return (
                number // (size_row * size_col),
                (number // size_col) % size_row,
                number % size_col,
            )

        def exists(step):
            a, b = step
            ok = None
            for delta, place, size in ((a, row, size_row), (b, col, size_col)):
                if delta:
                    this = place > 0 if delta < 0 else place < size - 1
                    ok = this if ok is None else jnp.logical_and(ok, this)
            return ok

        near = len(partners)
        for step in cross:
            near = near + exists(step).astype(jnp.int32)

        def greet():
            barrier = pltpu.get_barrier_semaphore()
            for other in partners:
                pl.semaphore_signal(
                    barrier, 1, device_id=((gz + other) % size_gz, row, col),
                    device_id_type=mesh_id,
                )
            for step in cross:
                @pl.when(exists(step))
                def _(step=step):
                    pl.semaphore_signal(
                        barrier, 1, device_id=(gz, row + step[0], col + step[1]),
                        device_id_type=mesh_id,
                    )


        greet()
        loads = [
            pltpu.make_async_copy(
                sec_hbm.at[n], ext.at[n, margin : margin + side, margin : margin + side],
                load_sem.at[n],
            )
            for n in range(2)
        ]
        tables = (
            (dft_hbm, dft_ref), (wg_hbm, wg_ref), (row_hbm, row_ref), (pri_hbm, pri_ref),
            (order_hbm, order_ref), (e_hbm, e_ref), (phase_hbm, phase_ref),
        )
        for n, (source, target) in enumerate(tables):
            loads.append(pltpu.make_async_copy(source, target, load_sem.at[n + 2]))
        for copy in loads:
            copy.start()

        def place(section, r0, rn, c0, cn):
            return ext.at[
                section, margin + r0 : margin + r0 + rn, margin + c0 : margin + c0 + cn
            ]

        def landing(n):
            section, _, (a, b), _, (r0, rn, c0, cn) = copies[n]
            return place(section, r0 - a * side, rn, c0 - b * side, cn)

        def halo_copy(n):
            section, _, (a, b), _, box = copies[n]
            return pltpu.make_async_remote_copy(
                src_ref=place(section, *box), dst_ref=landing(n),
                send_sem=halo_send.at[n], recv_sem=halo_recv.at[n],
                device_id=(gz, row + a, col + b), device_id_type=mesh_id,
            )

        def guard(n, sign):
            (a, b), side_col = copies[n][2], copies[n][3]
            return exists((sign * a, side_col if side_col else sign * b))

        def send(numbers):
            for n in numbers:
                @pl.when(guard(n, 1))
                def _(n=n):
                    halo_copy(n).start()

        def arrive(numbers):
            for n in numbers:
                @pl.when(guard(n, -1))
                def _(n=n):
                    ref = landing(n)
                    pltpu.make_async_copy(ref, ref, halo_recv.at[n]).wait()

        def chunk_copy(n):
            return pltpu.make_async_remote_copy(
                src_ref=place(0, *chunks[n]), dst_ref=place(2, *chunks[n]),
                send_sem=chunk_send.at[n], recv_sem=chunk_recv.at[n],
                device_id=((gz + size_gz - 1) % size_gz, row, col), device_id_type=mesh_id,
            )

        def took(low, high):
            for n in range(low, high):
                chunk_copy(n).wait_recv()

        def rung(n):
            if n < len(reaches):
                k = reaches[n]
                lines = []
                for way in (-k, k):
                    for axis, at, size in ((1, row, size_row), (2, col, size_col)):
                        ok = at + way >= 0 if way < 0 else at + way < size
                        lines.append((ok, (gz, row + way, col) if axis == 1 else (gz, row, col + way)))
                return lines
            if n == len(reaches):
                return [(None, (gz, row, (col + j) % size_col)) for j in range(1, size_col)]
            return [(None, ((gz + j) % size_gz, row, col)) for j in range(1, size_gz)]

        def climb(n):
            for ok, target in rung(n):
                def tell(target=target):
                    pl.semaphore_signal(
                        flood.at[n], 1, device_id=target, device_id_type=mesh_id
                    )
                if ok is None:
                    tell()
                else:
                    pl.when(ok)(tell)

        def heard(n):
            total = 0
            for ok, _ in rung(n):
                total = total + (1 if ok is None else ok.astype(jnp.int32))
            return total

        done = [0]

        def spread(upto):
            for n in range(done[0], min(upto, rounds)):
                pl.semaphore_wait(flood.at[n], heard(n))
                if n + 1 < rounds:
                    climb(n + 1)
            done[0] = max(done[0], min(upto, rounds))

        wide = ext.shape[2]
        edge, last = margin, wide - margin
        spans_of = {
            "middle": ((edge, last),),
            "outer": ((0, edge), (last, wide)),
            "sides": ((0, 2 * edge), (last - edge, wide)),
            "center": ((2 * edge, last - edge),),
        }

        def columns_pass(section, part):
            first_pass(ext, section, dft_ref, pq_ref, 2 * (section % 2), spans_of[part])

        lane = lax.broadcasted_iota(jnp.int32, (1, LAGS), 1)
        sections, columns = 2 * size_gz, 2 * size_col

        def prior(part, section, i, j):
            return pri_ref[part, section, i, j]

        def patch(section, i, j):
            phase = None
            if section < 2:
                phase = phase_ref[pl.ds(prior(1, section, i, j) + MAXOFF, 1), :]
            return spectrum_work(
                wg_ref, pq_ref, 2 * (section % 2) + i, j, turn_ref, 2 * i + j,
                cross_ref if section else None, phase,
            )

        def flows(section, surfaces):
            values = []
            for n in range(4):
                p, q = prior(0, section - 1, n // 2, n % 2), prior(1, section - 1, n // 2, n % 2)
                a, b = centroid(surfaces[n], p, q)
                at = (2 * gz + section - 1) * columns + 2 * col + n % 2
                value = jnp.where(lane == at, a, 0.0)
                values.append(value + jnp.where(lane == at + sections * columns, b, 0.0))
            mine_ref[0] = mine_ref[0] + values[0] + values[1]
            mine_ref[1] = mine_ref[1] + values[2] + values[3]

        def patches(section):
            halves, surfaces = {}, {}

            def spectra(i):
                return [patch(section, i, j) for j in range(2)]

            def half(i):
                return [half_work(cross_ref, 2 * i + j, e_ref, halves) for j in range(2)]

            def surface(i):
                for n in (2 * i, 2 * i + 1):
                    surfaces[n] = surface_of(halves[n], lags_ref[4 * (section - 1) + n])

            interleave(*spectra(0))
            if not section:
                interleave(*spectra(1))
                return
            interleave(*half(0), *spectra(1))
            interleave(*half(1))
            surface(0)
            surface(1)
            flows(section, surfaces)

        def lag_prepare(n, carry):
            lags_ref[n] = lag_rows(row_ref, prior(0, n // 4, (n // 2) % 2, n % 2))[:, : 2 * KROWS]
            return carry

        for step in cross + diagonal:
            @pl.when(jnp.logical_not(exists(step)))
            def _(step=step):
                (r0, rn), (c0, cn) = halo[step[0]], halo[step[1]]
                ext[:, margin + r0 : margin + r0 + rn, margin + c0 : margin + c0 + cn] = (
                    jnp.zeros((3, rn, cn), ext.dtype)
                )

        mine_ref[...] = jnp.zeros_like(mine_ref)
        pl.semaphore_wait(pltpu.get_barrier_semaphore(), near)
        loads[0].wait()
        for n in range(len(chunks)):
            chunk_copy(n).start()
        send(pick(0, "row", "col"))
        loads[1].wait()
        send(pick(1, "row", "col"))
        climb(0)
        for copy in loads[2:]:
            copy.wait()

        lax.fori_loop(0, 8, lag_prepare, 0)
        arrive(pick(0, "row"))
        columns_pass(0, "middle")
        spread(1)
        took(0, 4)
        send(pick(2, "diagonal", "corner"))
        arrive(pick(0, "col"))
        send(pick(0, "turn"))
        arrive(pick(1, "row"))
        columns_pass(1, "middle")
        spread(2)
        took(4, 5)
        send(pick(2, "left"))
        arrive(pick(1, "col"))
        send(pick(1, "turn"))
        took(5, 6)
        send(pick(2, "right"))
        arrive(pick(0, "turn"))
        columns_pass(0, "outer")
        patches(0)
        spread(3)
        took(6, 7)
        send(pick(2, "up"))
        took(7, 8)
        send(pick(2, "down"))
        arrive(pick(1, "turn"))
        columns_pass(1, "outer")
        patches(1)
        arrive(pick(2, "left", "right", "diagonal", "corner"))
        columns_pass(2, "sides")
        took(8, 9)
        arrive(pick(2, "up", "down"))
        columns_pass(2, "center")
        patches(2)
        spread(rounds)

        total_rows = 2 * size_row
        slot = gz * size_col + col
        spot = slot * total_rows + 2 * row

        rows_on = [(row + n) % size_row for n in range(size_row)]
        cols_on = [(col + n) % size_col for n in range(size_col)]
        for a in range(size_gz):
            plane = (gz + a) % size_gz
            for b in range(size_row):
                for c in range(size_col):
                    if a + b + c:
                        pltpu.make_async_remote_copy(
                            src_ref=mine_ref, dst_ref=all_ref.at[pl.ds(spot, 2)],
                            send_sem=flow_send, recv_sem=flow_recv,
                            device_id=(plane, rows_on[b], cols_on[c]), device_id_type=mesh_id,
                        ).start()
        all_ref[spot] = mine_ref[0]
        all_ref[spot + 1] = mine_ref[1]
        for n in range(len(chunks)):
            chunk_copy(n).wait_send()
        for n in range(len(copies)):
            @pl.when(guard(n, 1))
            def _(n=n):
                halo_copy(n).wait_send()
        got = all_ref.at[pl.ds(0, 2 * (count - 1))]
        pltpu.make_async_copy(got, got, flow_recv).wait()
        for m in range(rows_each):
            wanted = order_ref[row * rows_each + m]
            value = all_ref[wanted]
            for other in range(1, size_gz * size_col):
                value = value + all_ref[other * total_rows + wanted]
            out_ref[m : m + 1, :] = value[:, : out_ref.shape[1]]
        pltpu.make_async_copy(got, got, flow_send).wait()

    return kernel


def doubling(sizes):
    reaches = [1]
    while 2 * reaches[-1] < max(sizes[1:]):
        reaches.append(2 * reaches[-1])
    return reaches


def halo_copies(span, halo, margin, inner, cross, diagonal):
    copies = []
    for section in range(2):
        for step in cross:
            kind = "row" if step[0] else "col"
            copies.append((section, kind, step, 0, span[step[0]] + span[step[1]]))
        for a, b in diagonal:
            copies.append((section, "turn", (a, 0), b, span[a] + halo[b]))
    for a, b in diagonal:
        copies.append((2, "diagonal", (a, b), 0, span[a] + span[b]))
    for a, b in diagonal:
        copies.append((2, "corner", (a, 0), 0, span[a] + span[b]))
    for b in (-1, 1):
        copies.append((2, "left" if b < 0 else "right", (0, b), 0, span[0] + span[b]))
    for a in (-1, 1):
        copies.append((2, "up" if a < 0 else "down", (a, 0), 0, span[a] + (margin, inner)))
    return copies


def body(sections, priors, row_order):
    sizes = tuple(lax.axis_size(name) for name in ("gz", "row", "col"))
    count = math.prod(sizes)
    rows_each = row_order.shape[0] // sizes[1]
    width = 2 * 2 * sizes[0] * 2 * sizes[2]
    matrix, phase = column_tables()
    tables = (
        bf16_const(dft_table()),
        bf16_const(split_tables()),
        bf16_const(matrix),
        phase.astype(np.float32),
        f32_const(lane_tiles(lag_table())),
    )
    hbm = pl.BlockSpec(memory_space=pl.ANY)
    dma = pltpu.SemaphoreType.DMA
    wide = 2 * STRIDE + HALO
    flows = pl.pallas_call(
        make_kernel(sizes, rows_each),
        out_shape=jax.ShapeDtypeStruct((rows_each, width), jnp.float32),
        in_specs=[hbm] * 8,
        out_specs=pl.BlockSpec(memory_space=pltpu.VMEM),
        scratch_shapes=[
            pltpu.VMEM((3, wide, wide), jnp.bfloat16),
            *[pltpu.VMEM(t.shape, t.dtype) for t in tables],
            pltpu.VMEM((4, KROWS, 2 * PATCH), jnp.float32),
            pltpu.VMEM((4, KROWS, 2 * PATCH), jnp.bfloat16),
            pltpu.VMEM((8, LAGS, 2 * KROWS), jnp.bfloat16),
            pltpu.VMEM((4, 2 * KROWS, wide), jnp.float32),
            pltpu.VMEM((2, 1, LAGS), jnp.float32),
            pltpu.VMEM((2 * count, 1, LAGS), jnp.float32),
            dma((9,)), dma((28,)), dma((28,)), dma((9,)), dma((9,)), dma(()), dma(()),
            pltpu.SemaphoreType.REGULAR((len(doubling(sizes)) + 2,)),
            pltpu.SMEM(priors.shape, priors.dtype), pltpu.SMEM(row_order.shape, row_order.dtype),
        ],
        compiler_params=pltpu.CompilerParams(
            vmem_limit_bytes=41943040, collective_id=0, has_side_effects=True
        ),
    )(*[pltpu.with_memory_space_constraint(x, pltpu.HBM) for x in (priors, row_order, sections, *tables)])
    return flows


def solution(mesh):
    placed = (P("gz", "row", "col"), P(None, "gz", "row", "col"), P())
    return jax.shard_map(
        body, mesh=mesh, in_specs=placed, out_specs=P("row", None), check_vma=False
    )
```

```python
import math

import jax
import jax.numpy as jnp
import numpy as np
from jax import lax
from jax.experimental import pallas as pl
from jax.experimental.pallas import tpu as pltpu
from jax.sharding import PartitionSpec as P

PATCH = 512
STRIDE = 256
LAGS = 128
MAXOFF = 64
HALO = 256
HALF = PATCH // 2
QUARTER = PATCH // 4
KROWS = HALF + 16


def angle_of(products):
    return (products % PATCH) * (2.0 * math.pi / PATCH)


def dft_table():
    k = np.arange(HALF)[:, None]
    x = np.arange(PATCH)[None, :]
    table = np.zeros((2 * KROWS, PATCH))
    table[:HALF] = np.cos(angle_of(k * x))
    table[HALF] = np.cos(angle_of(HALF * x[0]))
    table[KROWS : KROWS + HALF] = -np.sin(angle_of(k * x))
    return table


def split_tables():
    y = np.arange(QUARTER)[:, None]
    blocks = []
    for g in range(4):
        l = 4 * np.arange(QUARTER)[None, :] + g
        c, s = np.cos(angle_of(y * l)), np.sin(angle_of(y * l))
        blocks.append(np.block([[c, -s], [s, c]]))
    return np.stack(blocks)


def lag_table():
    lag = np.arange(2 * LAGS)[:, None] - LAGS
    k = np.arange(KROWS)[None, :]
    weight = np.where(k == 0, 1.0, np.where(k < HALF, 2.0, np.where(k == HALF, 1.0, 0.0)))
    row_cos = np.cos(angle_of(lag * k)) * weight
    row_sin = -np.sin(angle_of(lag * k)) * weight
    return np.concatenate([row_cos, row_sin], axis=1)


def column_tables():
    lag = np.arange(LAGS)[None, :] - LAGS // 2
    shift = np.arange(-MAXOFF, MAXOFF + 1)[:, None]
    matrix, phase = [], []
    for g in range(4):
        l = 4 * np.arange(QUARTER) + g
        c, s = np.cos(angle_of(l[:, None] * lag)), np.sin(angle_of(l[:, None] * lag))
        matrix.append(np.block([[c, s], [-s, c]]))
        phase += [np.cos(angle_of(shift * l)), np.sin(angle_of(shift * l))]
    return np.concatenate(matrix), np.concatenate(phase, axis=1)


def bf16_const(value):
    return value.astype(np.float32).astype(jnp.bfloat16)


def f32_const(value):
    return bf16_const(value).astype(np.float32)


def first_pass(ext, section, dft_ref, pq_ref, slot, spans):
    boxes = [(i, low, high) for i in range(2) for low, high in spans]
    window = [ext[section, i * STRIDE : i * STRIDE + PATCH, low:high] for i, low, high in boxes]
    both = jnp.dot(
        dft_ref[...], jnp.concatenate(window, axis=1), preferred_element_type=jnp.float32
    )
    at = 0
    for i, low, high in boxes:
        pq_ref[slot + i, :, low:high] = both[:, at : at + high - low]
        at += high - low


def spectrum(wg_ref, pq_ref, slot, j):
    p, q = [], []
    for t in range(4):
        lanes = slice(j * STRIDE + t * QUARTER, j * STRIDE + (t + 1) * QUARTER)
        p.append(pq_ref[slot, :KROWS, lanes])
        q.append(pq_ref[slot, KROWS:, lanes])
    ps, pd, qs, qd = p[0] + p[2], p[0] - p[2], q[0] + q[2], q[0] - q[2]
    pt, pu, qt, qu = p[1] + p[3], p[1] - p[3], q[1] + q[3], q[1] - q[3]
    groups = ((ps + pt, qs + qt), (pd + qu, qd - pu), (ps - pt, qs - qt), (pd - qu, qd + pu))
    for g, (real, imag) in enumerate(groups):
        left = jnp.concatenate([real.astype(jnp.bfloat16), imag.astype(jnp.bfloat16)], axis=1)
        out = jnp.dot(left, wg_ref[g], preferred_element_type=jnp.float32)
        yield g, out[:, :QUARTER], out[:, QUARTER:]


def spectrum_work(wg_ref, pq_ref, slot, j, turn_ref, at, cross_ref, phase):
    for g, re, im in spectrum(wg_ref, pq_ref, slot, j):
        low, mid, high = 2 * g * QUARTER, (2 * g + 1) * QUARTER, (2 * g + 2) * QUARTER
        if cross_ref is not None:
            ar, ai = turn_ref[at, :, low:mid], turn_ref[at, :, mid:high]
            cross_ref[at, :, low:mid] = (ar * re + ai * im).astype(jnp.bfloat16)
            cross_ref[at, :, mid:high] = (ar * im - ai * re).astype(jnp.bfloat16)
        if phase is not None:
            c, s = phase[:, low:mid], phase[:, mid:high]
            turn_ref[at, :, low:mid] = re * c + im * s
            turn_ref[at, :, mid:high] = im * c - re * s
        yield


def lag_rows(table, prior):
    tiles = [
        table[t, pl.ds(prior + LAGS // 2, LAGS), :].astype(jnp.bfloat16)
        for t in range(table.shape[0])
    ]
    return jnp.concatenate(tiles, axis=1)


def lane_tiles(table):
    width = -(-table.shape[1] // LAGS) * LAGS
    table = np.pad(table, ((0, 0), (0, width - table.shape[1])))
    return np.stack(np.split(table, width // LAGS, axis=1))


def half_work(cross_ref, n, e_ref, halves):
    total = None
    for g in range(4):
        part = slice(2 * g * QUARTER, 2 * (g + 1) * QUARTER)
        piece = jnp.dot(cross_ref[n, :, part], e_ref[part], preferred_element_type=jnp.float32)
        total = piece if total is None else total + piece
        if g == 3:
            halves[n] = total.astype(jnp.bfloat16)
        yield


def surface_of(half, rows):
    stacked = jnp.concatenate([half[:, :LAGS], half[:, LAGS:]], axis=0)
    return jnp.dot(rows, stacked, preferred_element_type=jnp.float32) * (1.0 / PATCH**3)


def centroid(surface, p, q):
    f32 = jnp.float32
    w = surface * surface
    da = (lax.broadcasted_iota(jnp.int32, (LAGS, LAGS), 0) - LAGS // 2).astype(f32)
    db = (lax.broadcasted_iota(jnp.int32, (1, LAGS), 1) - LAGS // 2).astype(f32)
    col_w = jnp.sum(w, axis=0, keepdims=True)
    total = 1.0 + jnp.sum(col_w, axis=1, keepdims=True)
    row_m = jnp.sum(jnp.sum(w * da, axis=0, keepdims=True), axis=1, keepdims=True)
    col_m = jnp.sum(col_w * db, axis=1, keepdims=True)
    return p.astype(f32) + row_m / total, q.astype(f32) + col_m / total


def interleave(*works):
    for _ in zip(*works):
        pass


def make_kernel(sizes, rows_each):
    size_gz, size_row, size_col = sizes
    count = size_gz * size_row * size_col
    side = 2 * STRIDE
    margin = HALO // 2
    far = side - margin
    inner = far - margin
    mesh_id = pl.DeviceIdType.MESH
    cross = ((-1, 0), (1, 0), (0, -1), (0, 1))
    diagonal = ((-1, -1), (-1, 1), (1, -1), (1, 1))
    partners = sorted({1 % size_gz, size_gz - 1} - {0})
    reaches = doubling(sizes)
    rounds = len(reaches) + 2
    span = {-1: (0, margin), 0: (0, side), 1: (far, margin)}
    halo = {-1: (-margin, margin), 0: (0, side), 1: (side, margin)}
    chunks = (
        (0, margin, 0, margin), (0, margin, far, margin),
        (far, margin, 0, margin), (far, margin, far, margin),
        (margin, inner, 0, margin), (margin, inner, far, margin),
        (0, margin, margin, inner), (far, margin, margin, inner),
        (margin, inner, margin, inner),
    )
    copies = halo_copies(span, halo, margin, inner, cross, diagonal)

    def pick(section, *kinds):
        return [n for n, c in enumerate(copies) if c[0] == section and c[1] in kinds]

    def kernel(
        pri_hbm, order_hbm, sec_hbm, dft_hbm, wg_hbm, e_hbm, phase_hbm, row_hbm, out_ref,
        ext, dft_ref, wg_ref, e_ref, phase_ref, row_ref, turn_ref, cross_ref, lags_ref, pq_ref,
        mine_ref, all_ref,
        load_sem, halo_send, halo_recv, chunk_send, chunk_recv, flow_send, flow_recv, flood, pri_ref,
        order_ref,
    ):
        gz, row, col = lax.axis_index("gz"), lax.axis_index("row"), lax.axis_index("col")
        flat = (gz * size_row + row) * size_col + col

        def device(number):
            return (
                number // (size_row * size_col),
                (number // size_col) % size_row,
                number % size_col,
            )

        def exists(step):
            a, b = step
            ok = None
            for delta, place, size in ((a, row, size_row), (b, col, size_col)):
                if delta:
                    this = place > 0 if delta < 0 else place < size - 1
                    ok = this if ok is None else jnp.logical_and(ok, this)
            return ok

        near = len(partners)
        for step in cross:
            near = near + exists(step).astype(jnp.int32)

        def greet():
            barrier = pltpu.get_barrier_semaphore()
            for other in partners:
                pl.semaphore_signal(
                    barrier, 1, device_id=((gz + other) % size_gz, row, col),
                    device_id_type=mesh_id,
                )
            for step in cross:
                @pl.when(exists(step))
                def _(step=step):
                    pl.semaphore_signal(
                        barrier, 1, device_id=(gz, row + step[0], col + step[1]),
                        device_id_type=mesh_id,
                    )


        greet()
        loads = [
            pltpu.make_async_copy(
                sec_hbm.at[n], ext.at[n, margin : margin + side, margin : margin + side],
                load_sem.at[n],
            )
            for n in range(2)
        ]
        tables = (
            (dft_hbm, dft_ref), (wg_hbm, wg_ref), (row_hbm, row_ref), (pri_hbm, pri_ref),
            (order_hbm, order_ref), (e_hbm, e_ref), (phase_hbm, phase_ref),
        )
        for n, (source, target) in enumerate(tables):
            loads.append(pltpu.make_async_copy(source, target, load_sem.at[n + 2]))
        for copy in loads:
            copy.start()

        def place(section, r0, rn, c0, cn):
            return ext.at[
                section, margin + r0 : margin + r0 + rn, margin + c0 : margin + c0 + cn
            ]

        def landing(n):
            section, _, (a, b), _, (r0, rn, c0, cn) = copies[n]
            return place(section, r0 - a * side, rn, c0 - b * side, cn)

        def halo_copy(n):
            section, _, (a, b), _, box = copies[n]
            return pltpu.make_async_remote_copy(
                src_ref=place(section, *box), dst_ref=landing(n),
                send_sem=halo_send.at[n], recv_sem=halo_recv.at[n],
                device_id=(gz, row + a, col + b), device_id_type=mesh_id,
            )

        def guard(n, sign):
            _, kind, (a, b), side_col, _ = copies[n]
            if kind == "swing":
                return jnp.logical_and(row % 2 == 1, exists((1, sign * b)))
            ok = exists((sign * a, side_col if side_col else sign * b))
            if kind == "turn" and a < 0:
                ok = jnp.logical_and(ok, row % 2 == (1 if sign > 0 else 0))
            return ok

        def send(numbers):
            for n in numbers:
                @pl.when(guard(n, 1))
                def _(n=n):
                    halo_copy(n).start()

        def arrive(numbers):
            for n in numbers:
                @pl.when(guard(n, -1))
                def _(n=n):
                    ref = landing(n)
                    pltpu.make_async_copy(ref, ref, halo_recv.at[n]).wait()

        def chunk_copy(n):
            return pltpu.make_async_remote_copy(
                src_ref=place(0, *chunks[n]), dst_ref=place(2, *chunks[n]),
                send_sem=chunk_send.at[n], recv_sem=chunk_recv.at[n],
                device_id=((gz + size_gz - 1) % size_gz, row, col), device_id_type=mesh_id,
            )

        def took(low, high):
            for n in range(low, high):
                chunk_copy(n).wait_recv()

        def rung(n):
            if n < len(reaches):
                k = reaches[n]
                lines = []
                for way in (-k, k):
                    for axis, at, size in ((1, row, size_row), (2, col, size_col)):
                        ok = at + way >= 0 if way < 0 else at + way < size
                        lines.append((ok, (gz, row + way, col) if axis == 1 else (gz, row, col + way)))
                return lines
            if n == len(reaches):
                return [(None, (gz, row, (col + j) % size_col)) for j in range(1, size_col)]
            return [(None, ((gz + j) % size_gz, row, col)) for j in range(1, size_gz)]

        def climb(n):
            for ok, target in rung(n):
                def tell(target=target):
                    pl.semaphore_signal(
                        flood.at[n], 1, device_id=target, device_id_type=mesh_id
                    )
                if ok is None:
                    tell()
                else:
                    pl.when(ok)(tell)

        def heard(n):
            total = 0
            for ok, _ in rung(n):
                total = total + (1 if ok is None else ok.astype(jnp.int32))
            return total

        done = [0]

        def spread(upto):
            for n in range(done[0], min(upto, rounds)):
                pl.semaphore_wait(flood.at[n], heard(n))
                if n + 1 < rounds:
                    climb(n + 1)
            done[0] = max(done[0], min(upto, rounds))

        wide = ext.shape[2]
        edge, last = margin, wide - margin
        spans_of = {
            "middle": ((edge, last),),
            "outer": ((0, edge), (last, wide)),
            "sides": ((0, 2 * edge), (last - edge, wide)),
            "center": ((2 * edge, last - edge),),
        }

        def columns_pass(section, part):
            first_pass(ext, section, dft_ref, pq_ref, 2 * (section % 2), spans_of[part])

        lane = lax.broadcasted_iota(jnp.int32, (1, LAGS), 1)
        sections, columns = 2 * size_gz, 2 * size_col

        def prior(part, section, i, j):
            return pri_ref[part, section, i, j]

        def patch(section, i, j):
            phase = None
            if section < 2:
                phase = phase_ref[pl.ds(prior(1, section, i, j) + MAXOFF, 1), :]
            return spectrum_work(
                wg_ref, pq_ref, 2 * (section % 2) + i, j, turn_ref, 2 * i + j,
                cross_ref if section else None, phase,
            )

        def flows(section, surfaces):
            values = []
            for n in range(4):
                p, q = prior(0, section - 1, n // 2, n % 2), prior(1, section - 1, n // 2, n % 2)
                a, b = centroid(surfaces[n], p, q)
                at = (2 * gz + section - 1) * columns + 2 * col + n % 2
                value = jnp.where(lane == at, a, 0.0)
                values.append(value + jnp.where(lane == at + sections * columns, b, 0.0))
            mine_ref[0] = mine_ref[0] + values[0] + values[1]
            mine_ref[1] = mine_ref[1] + values[2] + values[3]

        def patches(section, event=None):
            halves, surfaces = {}, {}

            def spectra(i):
                return [patch(section, i, j) for j in range(2)]

            def half(i):
                return [half_work(cross_ref, 2 * i + j, e_ref, halves) for j in range(2)]

            def surface(i):
                for n in (2 * i, 2 * i + 1):
                    surfaces[n] = surface_of(halves[n], lags_ref[4 * (section - 1) + n])

            interleave(*spectra(0))
            if not section:
                interleave(*spectra(1))
                return
            if event is not None:
                event()
            interleave(*half(0), *spectra(1))
            interleave(*half(1))
            surface(0)
            surface(1)
            flows(section, surfaces)

        def lag_prepare(n, carry):
            lags_ref[n] = lag_rows(row_ref, prior(0, n // 4, (n // 2) % 2, n % 2))[:, : 2 * KROWS]
            return carry

        for step in cross + diagonal:
            @pl.when(jnp.logical_not(exists(step)))
            def _(step=step):
                (r0, rn), (c0, cn) = halo[step[0]], halo[step[1]]
                ext[:, margin + r0 : margin + r0 + rn, margin + c0 : margin + c0 + cn] = (
                    jnp.zeros((3, rn, cn), ext.dtype)
                )

        mine_ref[...] = jnp.zeros_like(mine_ref)
        pl.semaphore_wait(pltpu.get_barrier_semaphore(), near)
        loads[0].wait()
        for n in range(len(chunks)):
            chunk_copy(n).start()
        send(pick(0, "row", "col"))
        loads[1].wait()
        send(pick(1, "row", "col"))
        climb(0)
        for copy in loads[2:]:
            copy.wait()

        def top():
            took(6, 7)
            send(pick(2, "up"))

        def bottom():
            took(7, 8)
            send(pick(2, "down"))

        lax.fori_loop(0, 8, lag_prepare, 0)
        arrive(pick(0, "row"))
        send(pick(0, "swing"))
        columns_pass(0, "middle")
        spread(1)
        arrive(pick(0, "col"))
        send(pick(0, "turn"))
        arrive(pick(1, "row"))
        send(pick(1, "swing"))
        took(0, 4)
        send(pick(2, "diagonal", "corner"))
        columns_pass(1, "middle")
        spread(2)
        took(4, 5)
        send(pick(2, "left"))
        arrive(pick(1, "col"))
        send(pick(1, "turn"))
        took(5, 6)
        send(pick(2, "right"))
        arrive(pick(0, "turn", "swing"))
        columns_pass(0, "outer")
        patches(0)
        spread(3)
        top()
        arrive(pick(1, "turn", "swing"))
        columns_pass(1, "outer")
        patches(1, bottom)
        arrive(pick(2, "left", "right", "diagonal", "corner"))
        columns_pass(2, "sides")
        took(8, 9)
        arrive(pick(2, "up", "down"))
        columns_pass(2, "center")
        patches(2)
        spread(rounds)

        total_rows = 2 * size_row
        slot = gz * size_col + col
        spot = slot * total_rows + 2 * row

        rows_on = [(row + n) % size_row for n in range(size_row)]
        cols_on = [(col + n) % size_col for n in range(size_col)]
        for a in range(size_gz):
            plane = (gz + a) % size_gz
            for b in range(size_row):
                for c in range(size_col):
                    if a + b + c:
                        pltpu.make_async_remote_copy(
                            src_ref=mine_ref, dst_ref=all_ref.at[pl.ds(spot, 2)],
                            send_sem=flow_send, recv_sem=flow_recv,
                            device_id=(plane, rows_on[b], cols_on[c]), device_id_type=mesh_id,
                        ).start()
        all_ref[spot] = mine_ref[0]
        all_ref[spot + 1] = mine_ref[1]
        for n in range(len(chunks)):
            chunk_copy(n).wait_send()
        for n in range(len(copies)):
            @pl.when(guard(n, 1))
            def _(n=n):
                halo_copy(n).wait_send()
        got = all_ref.at[pl.ds(0, 2 * (count - 1))]
        pltpu.make_async_copy(got, got, flow_recv).wait()
        for m in range(rows_each):
            wanted = order_ref[row * rows_each + m]
            value = all_ref[wanted]
            for other in range(1, size_gz * size_col):
                value = value + all_ref[other * total_rows + wanted]
            out_ref[m : m + 1, :] = value[:, : out_ref.shape[1]]
        pltpu.make_async_copy(got, got, flow_send).wait()

    return kernel


def doubling(sizes):
    reaches = [1]
    while 2 * reaches[-1] < max(sizes[1:]):
        reaches.append(2 * reaches[-1])
    return reaches


def halo_copies(span, halo, margin, inner, cross, diagonal):
    copies = []
    for section in range(2):
        for step in cross:
            kind = "row" if step[0] else "col"
            copies.append((section, kind, step, 0, span[step[0]] + span[step[1]]))
        for a, b in diagonal:
            copies.append((section, "turn", (a, 0), b, span[a] + halo[b]))
        for b in (-1, 1):
            copies.append((section, "swing", (0, b), 0, halo[1] + span[b]))
    for a, b in diagonal:
        copies.append((2, "diagonal", (a, b), 0, span[a] + span[b]))
    for a, b in diagonal:
        copies.append((2, "corner", (a, 0), 0, span[a] + span[b]))
    for b in (-1, 1):
        copies.append((2, "left" if b < 0 else "right", (0, b), 0, span[0] + span[b]))
    for a in (-1, 1):
        copies.append((2, "up" if a < 0 else "down", (a, 0), 0, span[a] + (margin, inner)))
    return copies


def body(sections, priors, row_order):
    sizes = tuple(lax.axis_size(name) for name in ("gz", "row", "col"))
    count = math.prod(sizes)
    rows_each = row_order.shape[0] // sizes[1]
    width = 2 * 2 * sizes[0] * 2 * sizes[2]
    matrix, phase = column_tables()
    tables = (
        bf16_const(dft_table()),
        bf16_const(split_tables()),
        bf16_const(matrix),
        phase.astype(np.float32),
        f32_const(lane_tiles(lag_table())),
    )
    hbm = pl.BlockSpec(memory_space=pl.ANY)
    dma = pltpu.SemaphoreType.DMA
    wide = 2 * STRIDE + HALO
    flows = pl.pallas_call(
        make_kernel(sizes, rows_each),
        out_shape=jax.ShapeDtypeStruct((rows_each, width), jnp.float32),
        in_specs=[hbm] * 8,
        out_specs=pl.BlockSpec(memory_space=pltpu.VMEM),
        scratch_shapes=[
            pltpu.VMEM((3, wide, wide), jnp.bfloat16),
            *[pltpu.VMEM(t.shape, t.dtype) for t in tables],
            pltpu.VMEM((4, KROWS, 2 * PATCH), jnp.float32),
            pltpu.VMEM((4, KROWS, 2 * PATCH), jnp.bfloat16),
            pltpu.VMEM((8, LAGS, 2 * KROWS), jnp.bfloat16),
            pltpu.VMEM((4, 2 * KROWS, wide), jnp.float32),
            pltpu.VMEM((2, 1, LAGS), jnp.float32),
            pltpu.VMEM((2 * count, 1, LAGS), jnp.float32),
            dma((9,)), dma((32,)), dma((32,)), dma((9,)), dma((9,)), dma(()), dma(()),
            pltpu.SemaphoreType.REGULAR((len(doubling(sizes)) + 2,)),
            pltpu.SMEM(priors.shape, priors.dtype), pltpu.SMEM(row_order.shape, row_order.dtype),
        ],
        compiler_params=pltpu.CompilerParams(
            vmem_limit_bytes=41943040, collective_id=0, has_side_effects=True
        ),
    )(*[pltpu.with_memory_space_constraint(x, pltpu.HBM) for x in (priors, row_order, sections, *tables)])
    return flows


def solution(mesh):
    placed = (P("gz", "row", "col"), P(None, "gz", "row", "col"), P())
    return jax.shard_map(
        body, mesh=mesh, in_specs=placed, out_specs=P("row", None), check_vma=False
    )
```

```python
import math

import jax
import jax.numpy as jnp
import numpy as np
from jax import lax
from jax.experimental import pallas as pl
from jax.experimental.pallas import tpu as pltpu
from jax.sharding import PartitionSpec as P

PATCH = 512
STRIDE = 256
LAGS = 128
HALO = 256
HALF = PATCH // 2
QUARTER = PATCH // 4
KROWS = HALF + 16


def angle_of(products):
    return (products % PATCH) * (2.0 * math.pi / PATCH)


def dft_table():
    k = np.arange(HALF)[:, None]
    x = np.arange(PATCH)[None, :]
    table = np.zeros((2 * KROWS, PATCH))
    table[:HALF] = np.cos(angle_of(k * x))
    table[HALF] = np.cos(angle_of(HALF * x[0]))
    table[KROWS : KROWS + HALF] = -np.sin(angle_of(k * x))
    return table


def split_tables():
    y = np.arange(QUARTER)[:, None]
    blocks = []
    for g in range(4):
        l = 4 * np.arange(QUARTER)[None, :] + g
        c, s = np.cos(angle_of(y * l)), np.sin(angle_of(y * l))
        blocks.append(np.block([[c, -s], [s, c]]))
    return np.stack(blocks)


def lag_table():
    lag = np.arange(2 * LAGS)[:, None] - LAGS
    k = np.arange(KROWS)[None, :]
    weight = np.where(k == 0, 1.0, np.where(k < HALF, 2.0, np.where(k == HALF, 1.0, 0.0)))
    row_cos = np.cos(angle_of(lag * k)) * weight
    row_sin = -np.sin(angle_of(lag * k)) * weight
    return np.concatenate([row_cos, row_sin], axis=1)


def column_tables():
    lag = np.arange(2 * LAGS)[:, None] - LAGS
    l = np.concatenate([4 * np.arange(QUARTER) + g for g in range(4)])[None, :]
    return np.cos(angle_of(lag * l)), np.sin(angle_of(lag * l))


def bf16_const(value):
    return value.astype(np.float32).astype(jnp.bfloat16)


def f32_const(value):
    return bf16_const(value).astype(np.float32)


def first_pass(ext, section, dft_ref, pq_ref, slot, spans):
    boxes = [(i, low, high) for i in range(2) for low, high in spans]
    window = [ext[section, i * STRIDE : i * STRIDE + PATCH, low:high] for i, low, high in boxes]
    both = jnp.dot(
        dft_ref[...], jnp.concatenate(window, axis=1), preferred_element_type=jnp.float32
    )
    at = 0
    for i, low, high in boxes:
        pq_ref[slot + i, :, low:high] = both[:, at : at + high - low]
        at += high - low


def spectrum(wg_ref, pq_ref, slot, j):
    p, q = [], []
    for t in range(4):
        lanes = slice(j * STRIDE + t * QUARTER, j * STRIDE + (t + 1) * QUARTER)
        p.append(pq_ref[slot, :KROWS, lanes])
        q.append(pq_ref[slot, KROWS:, lanes])
    ps, pd, qs, qd = p[0] + p[2], p[0] - p[2], q[0] + q[2], q[0] - q[2]
    pt, pu, qt, qu = p[1] + p[3], p[1] - p[3], q[1] + q[3], q[1] - q[3]
    groups = ((ps + pt, qs + qt), (pd + qu, qd - pu), (ps - pt, qs - qt), (pd - qu, qd + pu))
    for g, (real, imag) in enumerate(groups):
        left = jnp.concatenate([real.astype(jnp.bfloat16), imag.astype(jnp.bfloat16)], axis=1)
        out = jnp.dot(left, wg_ref[g], preferred_element_type=jnp.float32)
        yield g, out[:, :QUARTER], out[:, QUARTER:]


def spectrum_work(wg_ref, pq_ref, slot, j, first_ref, at, cross_ref, keep):
    for g, re, im in spectrum(wg_ref, pq_ref, slot, j):
        low, mid, high = 2 * g * QUARTER, (2 * g + 1) * QUARTER, (2 * g + 2) * QUARTER
        if cross_ref is not None:
            ar, ai = first_ref[at, :, low:mid], first_ref[at, :, mid:high]
            cross_ref[at, :, low:mid] = (ar * re + ai * im).astype(jnp.bfloat16)
            cross_ref[at, :, mid:high] = (ar * im - ai * re).astype(jnp.bfloat16)
        if keep:
            first_ref[at, :, low:mid] = re
            first_ref[at, :, mid:high] = im
        yield


def lag_rows(table, prior):
    tiles = [
        table[t, pl.ds(prior + LAGS // 2, LAGS), :].astype(jnp.bfloat16)
        for t in range(table.shape[0])
    ]
    return jnp.concatenate(tiles, axis=1)


def lane_tiles(table):
    width = -(-table.shape[1] // LAGS) * LAGS
    table = np.pad(table, ((0, 0), (0, width - table.shape[1])))
    return np.stack(np.split(table, width // LAGS, axis=1))


def half_work(cross_ref, n, e_ref, pair, halves):
    total = None
    for g in range(4):
        part = slice(2 * g * QUARTER, 2 * (g + 1) * QUARTER)
        piece = lax.dot_general(
            cross_ref[n, :, part], e_ref[pair, :, part], (((1,), (1,)), ((), ())),
            preferred_element_type=jnp.float32,
        )
        total = piece if total is None else total + piece
        if g == 3:
            halves[n] = total.astype(jnp.bfloat16)
        yield


def surface_of(half, rows):
    stacked = jnp.concatenate([half[:, :LAGS], half[:, LAGS:]], axis=0)
    return jnp.dot(rows, stacked, preferred_element_type=jnp.float32) * (1.0 / PATCH**3)


def centroid(surface, p, q):
    f32 = jnp.float32
    w = surface * surface
    da = (lax.broadcasted_iota(jnp.int32, (LAGS, LAGS), 0) - LAGS // 2).astype(f32)
    db = (lax.broadcasted_iota(jnp.int32, (1, LAGS), 1) - LAGS // 2).astype(f32)
    col_w = jnp.sum(w, axis=0, keepdims=True)
    total = 1.0 + jnp.sum(col_w, axis=1, keepdims=True)
    row_m = jnp.sum(jnp.sum(w * da, axis=0, keepdims=True), axis=1, keepdims=True)
    col_m = jnp.sum(col_w * db, axis=1, keepdims=True)
    return p.astype(f32) + row_m / total, q.astype(f32) + col_m / total


def interleave(*works):
    for _ in zip(*works):
        pass


def make_kernel(sizes, rows_each):
    size_gz, size_row, size_col = sizes
    count = size_gz * size_row * size_col
    side = 2 * STRIDE
    margin = HALO // 2
    far = side - margin
    inner = far - margin
    mesh_id = pl.DeviceIdType.MESH
    cross = ((-1, 0), (1, 0), (0, -1), (0, 1))
    diagonal = ((-1, -1), (-1, 1), (1, -1), (1, 1))
    partners = sorted({1 % size_gz, size_gz - 1} - {0})
    reaches = doubling(sizes)
    rounds = len(reaches) + 2
    span = {-1: (0, margin), 0: (0, side), 1: (far, margin)}
    halo = {-1: (-margin, margin), 0: (0, side), 1: (side, margin)}
    chunks = (
        (0, margin, 0, margin), (0, margin, far, margin),
        (far, margin, 0, margin), (far, margin, far, margin),
        (margin, inner, 0, margin), (margin, inner, far, margin),
        (0, margin, margin, inner), (far, margin, margin, inner),
        (margin, inner, margin, inner),
    )
    copies = halo_copies(span, halo, margin, inner, cross, diagonal)

    def pick(section, *kinds):
        return [n for n, c in enumerate(copies) if c[0] == section and c[1] in kinds]

    def kernel(
        pri_hbm, order_hbm, sec_hbm, dft_hbm, wg_hbm, colc_hbm, cols_hbm, row_hbm, out_ref,
        ext, dft_ref, wg_ref, colc_ref, cols_ref, row_ref, first_ref, cross_ref, lags_ref, e_ref,
        pq_ref,
        mine_ref, all_ref,
        load_sem, halo_send, halo_recv, chunk_send, chunk_recv, flow_send, flow_recv, flood, pri_ref,
        order_ref,
    ):
        gz, row, col = lax.axis_index("gz"), lax.axis_index("row"), lax.axis_index("col")
        flat = (gz * size_row + row) * size_col + col

        def device(number):
            return (
                number // (size_row * size_col),
                (number // size_col) % size_row,
                number % size_col,
            )

        def exists(step):
            a, b = step
            ok = None
            for delta, place, size in ((a, row, size_row), (b, col, size_col)):
                if delta:
                    this = place > 0 if delta < 0 else place < size - 1
                    ok = this if ok is None else jnp.logical_and(ok, this)
            return ok

        near = len(partners)
        for step in cross:
            near = near + exists(step).astype(jnp.int32)

        def greet():
            barrier = pltpu.get_barrier_semaphore()
            for other in partners:
                pl.semaphore_signal(
                    barrier, 1, device_id=((gz + other) % size_gz, row, col),
                    device_id_type=mesh_id,
                )
            for step in cross:
                @pl.when(exists(step))
                def _(step=step):
                    pl.semaphore_signal(
                        barrier, 1, device_id=(gz, row + step[0], col + step[1]),
                        device_id_type=mesh_id,
                    )


        greet()
        loads = [
            pltpu.make_async_copy(
                sec_hbm.at[n], ext.at[n, margin : margin + side, margin : margin + side],
                load_sem.at[n],
            )
            for n in range(2)
        ]
        tables = (
            (dft_hbm, dft_ref), (wg_hbm, wg_ref), (row_hbm, row_ref), (pri_hbm, pri_ref),
            (order_hbm, order_ref), (colc_hbm, colc_ref), (cols_hbm, cols_ref),
        )
        for n, (source, target) in enumerate(tables):
            loads.append(pltpu.make_async_copy(source, target, load_sem.at[n + 2]))
        for copy in loads:
            copy.start()

        def place(section, r0, rn, c0, cn):
            return ext.at[
                section, margin + r0 : margin + r0 + rn, margin + c0 : margin + c0 + cn
            ]

        def landing(n):
            section, _, (a, b), _, (r0, rn, c0, cn) = copies[n]
            return place(section, r0 - a * side, rn, c0 - b * side, cn)

        def halo_copy(n):
            section, _, (a, b), _, box = copies[n]
            return pltpu.make_async_remote_copy(
                src_ref=place(section, *box), dst_ref=landing(n),
                send_sem=halo_send.at[n], recv_sem=halo_recv.at[n],
                device_id=(gz, row + a, col + b), device_id_type=mesh_id,
            )

        def guard(n, sign):
            _, kind, (a, b), side_col, _ = copies[n]
            if kind == "swing":
                return jnp.logical_and(row % 2 == 1, exists((1, sign * b)))
            ok = exists((sign * a, side_col if side_col else sign * b))
            if kind == "turn" and a < 0:
                ok = jnp.logical_and(ok, row % 2 == (1 if sign > 0 else 0))
            return ok

        def send(numbers):
            for n in numbers:
                @pl.when(guard(n, 1))
                def _(n=n):
                    halo_copy(n).start()

        def arrive(numbers):
            for n in numbers:
                @pl.when(guard(n, -1))
                def _(n=n):
                    ref = landing(n)
                    pltpu.make_async_copy(ref, ref, halo_recv.at[n]).wait()

        def chunk_copy(n):
            return pltpu.make_async_remote_copy(
                src_ref=place(0, *chunks[n]), dst_ref=place(2, *chunks[n]),
                send_sem=chunk_send.at[n], recv_sem=chunk_recv.at[n],
                device_id=((gz + size_gz - 1) % size_gz, row, col), device_id_type=mesh_id,
            )

        def took(low, high):
            for n in range(low, high):
                chunk_copy(n).wait_recv()

        def rung(n):
            if n < len(reaches):
                k = reaches[n]
                lines = []
                for way in (-k, k):
                    for axis, at, size in ((1, row, size_row), (2, col, size_col)):
                        ok = at + way >= 0 if way < 0 else at + way < size
                        lines.append((ok, (gz, row + way, col) if axis == 1 else (gz, row, col + way)))
                return lines
            if n == len(reaches):
                return [(None, (gz, row, (col + j) % size_col)) for j in range(1, size_col)]
            return [(None, ((gz + j) % size_gz, row, col)) for j in range(1, size_gz)]

        def climb(n):
            for ok, target in rung(n):
                def tell(target=target):
                    pl.semaphore_signal(
                        flood.at[n], 1, device_id=target, device_id_type=mesh_id
                    )
                if ok is None:
                    tell()
                else:
                    pl.when(ok)(tell)

        def heard(n):
            total = 0
            for ok, _ in rung(n):
                total = total + (1 if ok is None else ok.astype(jnp.int32))
            return total

        done = [0]

        def spread(upto):
            for n in range(done[0], min(upto, rounds)):
                pl.semaphore_wait(flood.at[n], heard(n))
                if n + 1 < rounds:
                    climb(n + 1)
            done[0] = max(done[0], min(upto, rounds))

        wide = ext.shape[2]
        edge, last = margin, wide - margin
        spans_of = {
            "middle": ((edge, last),),
            "outer": ((0, edge), (last, wide)),
            "sides": ((0, 2 * edge), (last - edge, wide)),
            "center": ((2 * edge, last - edge),),
        }

        def columns_pass(section, part):
            first_pass(ext, section, dft_ref, pq_ref, 2 * (section % 2), spans_of[part])

        lane = lax.broadcasted_iota(jnp.int32, (1, LAGS), 1)
        sections, columns = 2 * size_gz, 2 * size_col

        def prior(part, section, i, j):
            return pri_ref[part, section, i, j]

        def patch(section, i, j):
            return spectrum_work(
                wg_ref, pq_ref, 2 * (section % 2) + i, j, first_ref, 2 * i + j,
                cross_ref if section else None, section < 2,
            )

        def flows(section, surfaces):
            values = []
            for n in range(4):
                p, q = prior(0, section - 1, n // 2, n % 2), prior(1, section - 1, n // 2, n % 2)
                a, b = centroid(surfaces[n], p, q)
                at = (2 * gz + section - 1) * columns + 2 * col + n % 2
                value = jnp.where(lane == at, a, 0.0)
                values.append(value + jnp.where(lane == at + sections * columns, b, 0.0))
            mine_ref[0] = mine_ref[0] + values[0] + values[1]
            mine_ref[1] = mine_ref[1] + values[2] + values[3]

        def patches(section, event=None):
            halves, surfaces = {}, {}

            def spectra(i):
                return [patch(section, i, j) for j in range(2)]

            def half(i):
                return [
                    half_work(cross_ref, n, e_ref, 4 * (section - 1) + n, halves)
                    for n in (2 * i, 2 * i + 1)
                ]

            def surface(i):
                for n in (2 * i, 2 * i + 1):
                    surfaces[n] = surface_of(halves[n], lags_ref[4 * (section - 1) + n])

            interleave(*spectra(0))
            if not section:
                interleave(*spectra(1))
                return
            if event is not None:
                event()
            interleave(*half(0), *spectra(1))
            interleave(*half(1))
            surface(0)
            surface(1)
            flows(section, surfaces)

        def lag_prepare(n, carry):
            lags_ref[n] = lag_rows(row_ref, prior(0, n // 4, (n // 2) % 2, n % 2))[:, : 2 * KROWS]
            shift = prior(1, n // 4, (n // 2) % 2, n % 2) + LAGS // 2
            for g in range(4):
                ec = colc_ref[g, pl.ds(shift, LAGS), :]
                es = cols_ref[g, pl.ds(shift, LAGS), :]
                tiles = ((ec, -es), (es, ec))
                for a in range(2):
                    for b in range(2):
                        at = (2 * g + b) * QUARTER
                        e_ref[n, a * LAGS : (a + 1) * LAGS, at : at + QUARTER] = tiles[a][b].astype(
                            jnp.bfloat16
                        )
            return carry

        for step in cross + diagonal:
            @pl.when(jnp.logical_not(exists(step)))
            def _(step=step):
                (r0, rn), (c0, cn) = halo[step[0]], halo[step[1]]
                ext[:, margin + r0 : margin + r0 + rn, margin + c0 : margin + c0 + cn] = (
                    jnp.zeros((3, rn, cn), ext.dtype)
                )

        mine_ref[...] = jnp.zeros_like(mine_ref)
        pl.semaphore_wait(pltpu.get_barrier_semaphore(), near)
        loads[0].wait()
        for n in range(len(chunks)):
            chunk_copy(n).start()
        send(pick(0, "row", "col"))
        loads[1].wait()
        send(pick(1, "row", "col"))
        climb(0)
        for copy in loads[2:]:
            copy.wait()

        def top():
            took(6, 7)
            send(pick(2, "up"))

        def bottom():
            took(7, 8)
            send(pick(2, "down"))

        lax.fori_loop(0, 8, lag_prepare, 0)
        arrive(pick(0, "row"))
        send(pick(0, "swing"))
        columns_pass(0, "middle")
        spread(1)
        arrive(pick(0, "col"))
        send(pick(0, "turn"))
        arrive(pick(1, "row"))
        send(pick(1, "swing"))
        took(0, 4)
        send(pick(2, "diagonal", "corner"))
        columns_pass(1, "middle")
        spread(2)
        took(4, 5)
        send(pick(2, "left"))
        arrive(pick(1, "col"))
        send(pick(1, "turn"))
        took(5, 6)
        send(pick(2, "right"))
        arrive(pick(0, "turn", "swing"))
        columns_pass(0, "outer")
        patches(0)
        spread(3)
        top()
        arrive(pick(1, "turn", "swing"))
        columns_pass(1, "outer")
        patches(1, bottom)
        arrive(pick(2, "left", "right", "diagonal", "corner"))
        columns_pass(2, "sides")
        took(8, 9)
        arrive(pick(2, "up", "down"))
        columns_pass(2, "center")
        patches(2)
        spread(rounds)

        total_rows = 2 * size_row
        slot = gz * size_col + col
        spot = slot * total_rows + 2 * row

        rows_on = [(row + n) % size_row for n in range(size_row)]
        cols_on = [(col + n) % size_col for n in range(size_col)]
        for a in range(size_gz):
            plane = (gz + a) % size_gz
            for b in range(size_row):
                for c in range(size_col):
                    if a + b + c:
                        pltpu.make_async_remote_copy(
                            src_ref=mine_ref, dst_ref=all_ref.at[pl.ds(spot, 2)],
                            send_sem=flow_send, recv_sem=flow_recv,
                            device_id=(plane, rows_on[b], cols_on[c]), device_id_type=mesh_id,
                        ).start()
        all_ref[spot] = mine_ref[0]
        all_ref[spot + 1] = mine_ref[1]
        for n in range(len(chunks)):
            chunk_copy(n).wait_send()
        for n in range(len(copies)):
            @pl.when(guard(n, 1))
            def _(n=n):
                halo_copy(n).wait_send()
        got = all_ref.at[pl.ds(0, 2 * (count - 1))]
        pltpu.make_async_copy(got, got, flow_recv).wait()
        for m in range(rows_each):
            wanted = order_ref[row * rows_each + m]
            value = all_ref[wanted]
            for other in range(1, size_gz * size_col):
                value = value + all_ref[other * total_rows + wanted]
            out_ref[m : m + 1, :] = value[:, : out_ref.shape[1]]
        pltpu.make_async_copy(got, got, flow_send).wait()

    return kernel


def doubling(sizes):
    reaches = [1]
    while 2 * reaches[-1] < max(sizes[1:]):
        reaches.append(2 * reaches[-1])
    return reaches


def halo_copies(span, halo, margin, inner, cross, diagonal):
    copies = []
    for section in range(2):
        for step in cross:
            kind = "row" if step[0] else "col"
            copies.append((section, kind, step, 0, span[step[0]] + span[step[1]]))
        for a, b in diagonal:
            copies.append((section, "turn", (a, 0), b, span[a] + halo[b]))
        for b in (-1, 1):
            copies.append((section, "swing", (0, b), 0, halo[1] + span[b]))
    for a, b in diagonal:
        copies.append((2, "diagonal", (a, b), 0, span[a] + span[b]))
    for a, b in diagonal:
        copies.append((2, "corner", (a, 0), 0, span[a] + span[b]))
    for b in (-1, 1):
        copies.append((2, "left" if b < 0 else "right", (0, b), 0, span[0] + span[b]))
    for a in (-1, 1):
        copies.append((2, "up" if a < 0 else "down", (a, 0), 0, span[a] + (margin, inner)))
    return copies


def body(sections, priors, row_order):
    sizes = tuple(lax.axis_size(name) for name in ("gz", "row", "col"))
    count = math.prod(sizes)
    rows_each = row_order.shape[0] // sizes[1]
    width = 2 * 2 * sizes[0] * 2 * sizes[2]
    colc, cols = column_tables()
    tables = (
        bf16_const(dft_table()),
        bf16_const(split_tables()),
        f32_const(lane_tiles(colc)),
        f32_const(lane_tiles(cols)),
        f32_const(lane_tiles(lag_table())),
    )
    hbm = pl.BlockSpec(memory_space=pl.ANY)
    dma = pltpu.SemaphoreType.DMA
    wide = 2 * STRIDE + HALO
    flows = pl.pallas_call(
        make_kernel(sizes, rows_each),
        out_shape=jax.ShapeDtypeStruct((rows_each, width), jnp.float32),
        in_specs=[hbm] * 8,
        out_specs=pl.BlockSpec(memory_space=pltpu.VMEM),
        scratch_shapes=[
            pltpu.VMEM((3, wide, wide), jnp.bfloat16),
            *[pltpu.VMEM(t.shape, t.dtype) for t in tables],
            pltpu.VMEM((4, KROWS, 2 * PATCH), jnp.float32),
            pltpu.VMEM((4, KROWS, 2 * PATCH), jnp.bfloat16),
            pltpu.VMEM((8, LAGS, 2 * KROWS), jnp.bfloat16),
            pltpu.VMEM((8, 2 * LAGS, 2 * PATCH), jnp.bfloat16),
            pltpu.VMEM((4, 2 * KROWS, wide), jnp.float32),
            pltpu.VMEM((2, 1, LAGS), jnp.float32),
            pltpu.VMEM((2 * count, 1, LAGS), jnp.float32),
            dma((9,)), dma((32,)), dma((32,)), dma((9,)), dma((9,)), dma(()), dma(()),
            pltpu.SemaphoreType.REGULAR((len(doubling(sizes)) + 2,)),
            pltpu.SMEM(priors.shape, priors.dtype), pltpu.SMEM(row_order.shape, row_order.dtype),
        ],
        compiler_params=pltpu.CompilerParams(
            vmem_limit_bytes=41943040, collective_id=0, has_side_effects=True,
        ),
    )(*[pltpu.with_memory_space_constraint(x, pltpu.HBM) for x in (priors, row_order, sections, *tables)])
    return flows


def solution(mesh):
    placed = (P("gz", "row", "col"), P(None, "gz", "row", "col"), P())
    return jax.shard_map(
        body, mesh=mesh, in_specs=placed, out_specs=P("row", None), check_vma=False
    )
```

```python
import math

import jax
import jax.numpy as jnp
import numpy as np
from jax import lax
from jax.experimental import pallas as pl
from jax.experimental.pallas import tpu as pltpu
from jax.sharding import PartitionSpec as P

PATCH = 512
STRIDE = 256
LAGS = 128
HALO = 256
HALF = PATCH // 2
QUARTER = PATCH // 4
KROWS = HALF + 16
BLOCK = 16


def angle_of(products):
    return (products % PATCH) * (2.0 * math.pi / PATCH)


def dft_table():
    k = np.arange(HALF)[:, None]
    x = np.arange(PATCH)[None, :]
    cosine, sine = np.zeros((KROWS, PATCH)), np.zeros((KROWS, PATCH))
    cosine[:HALF] = np.cos(angle_of(k * x))
    cosine[HALF] = np.cos(angle_of(HALF * x[0]))
    sine[:HALF] = -np.sin(angle_of(k * x))
    blocks = np.stack([cosine.reshape(-1, BLOCK, PATCH), sine.reshape(-1, BLOCK, PATCH)], axis=1)
    return blocks.reshape(2 * KROWS, PATCH)


def split_tables():
    y = np.arange(QUARTER)[:, None]
    blocks = []
    for g in range(4):
        l = 4 * np.arange(QUARTER)[None, :] + g
        c, s = np.cos(angle_of(y * l)), np.sin(angle_of(y * l))
        blocks.append(np.block([[c, -s], [s, c]]))
    return np.stack(blocks)


def lag_table():
    lag = np.arange(2 * LAGS)[:, None] - LAGS
    k = np.arange(KROWS)[None, :]
    weight = np.where(k == 0, 1.0, np.where(k < HALF, 2.0, np.where(k == HALF, 1.0, 0.0)))
    row_cos = np.cos(angle_of(lag * k)) * weight
    row_sin = -np.sin(angle_of(lag * k)) * weight
    row_sin[:, 0] = row_cos[:, HALF]
    return np.concatenate([row_cos[:, :HALF], row_sin[:, :HALF]], axis=1)


def column_tables():
    lag = np.arange(2 * LAGS)[:, None] - LAGS
    l = np.concatenate([4 * np.arange(QUARTER) + g for g in range(4)])[None, :]
    return np.cos(angle_of(lag * l)), np.sin(angle_of(lag * l))


def bf16_const(value):
    return value.astype(np.float32).astype(jnp.bfloat16)


def f32_const(value):
    return bf16_const(value).astype(np.float32)


def first_pass(ext, section, dft_ref, pq_ref, slot, spans):
    boxes = [(i, low, high) for i in range(2) for low, high in spans]
    window = [ext[section, i * STRIDE : i * STRIDE + PATCH, low:high] for i, low, high in boxes]
    both = jnp.dot(
        dft_ref[...], jnp.concatenate(window, axis=1), preferred_element_type=jnp.float32
    )
    at = 0
    for i, low, high in boxes:
        pq_ref[slot + i, :, low:high] = both[:, at : at + high - low]
        at += high - low


def spectrum(wg_ref, pq_ref, slot, j):
    p, q = [], []
    for t in range(4):
        lanes = slice(j * STRIDE + t * QUARTER, j * STRIDE + (t + 1) * QUARTER)
        rows = [pq_ref[slot, low : low + BLOCK, lanes] for low in range(0, 2 * KROWS, BLOCK)]
        p.append(jnp.concatenate(rows[0::2], axis=0))
        q.append(jnp.concatenate(rows[1::2], axis=0))
    ps, pd, qs, qd = p[0] + p[2], p[0] - p[2], q[0] + q[2], q[0] - q[2]
    pt, pu, qt, qu = p[1] + p[3], p[1] - p[3], q[1] + q[3], q[1] - q[3]
    groups = ((ps + pt, qs + qt), (pd + qu, qd - pu), (ps - pt, qs - qt), (pd - qu, qd + pu))
    for g, (real, imag) in enumerate(groups):
        left = jnp.concatenate([real.astype(jnp.bfloat16), imag.astype(jnp.bfloat16)], axis=1)
        out = jnp.dot(left, wg_ref[g], preferred_element_type=jnp.float32)
        yield g, out[:, :QUARTER], out[:, QUARTER:]


def spectrum_work(wg_ref, pq_ref, slot, j, first_ref, at, cross_ref, keep):
    for g, re, im in spectrum(wg_ref, pq_ref, slot, j):
        low, mid, high = 2 * g * QUARTER, (2 * g + 1) * QUARTER, (2 * g + 2) * QUARTER
        if cross_ref is not None:
            ar, ai = first_ref[at, :, low:mid], first_ref[at, :, mid:high]
            cross_ref[at, :, low:mid] = (ar * re + ai * im).astype(jnp.bfloat16)
            cross_ref[at, :, mid:high] = (ar * im - ai * re).astype(jnp.bfloat16)
        if keep:
            first_ref[at, :, low:mid] = re
            first_ref[at, :, mid:high] = im
        yield


def lag_rows(table, prior):
    tiles = [
        table[t, pl.ds(prior + LAGS // 2, LAGS), :].astype(jnp.bfloat16)
        for t in range(table.shape[0])
    ]
    return jnp.concatenate(tiles, axis=1)


def lane_tiles(table):
    width = -(-table.shape[1] // LAGS) * LAGS
    table = np.pad(table, ((0, 0), (0, width - table.shape[1])))
    return np.stack(np.split(table, width // LAGS, axis=1))


def half_work(cross_ref, n, e_ref, pair, halves):
    total = None
    for g in range(4):
        part = slice(2 * g * QUARTER, 2 * (g + 1) * QUARTER)
        piece = lax.dot_general(
            cross_ref[n, :, part], e_ref[pair, :, part], (((1,), (1,)), ((), ())),
            preferred_element_type=jnp.float32,
        )
        total = piece if total is None else total + piece
        if g == 3:
            halves[n] = total.astype(jnp.bfloat16)
        yield


def surface_of(half, rows):
    first = lax.broadcasted_iota(jnp.int32, (BLOCK, LAGS), 0) == 0
    head = jnp.where(first, half[HALF:, :LAGS], half[:BLOCK, LAGS:])
    stacked = jnp.concatenate([half[:HALF, :LAGS], head, half[BLOCK:HALF, LAGS:]], axis=0)
    return jnp.dot(rows, stacked, preferred_element_type=jnp.float32) * (1.0 / PATCH**3)


def centroid(surface, p, q):
    f32 = jnp.float32
    w = surface * surface
    da = (lax.broadcasted_iota(jnp.int32, (LAGS, LAGS), 0) - LAGS // 2).astype(f32)
    db = (lax.broadcasted_iota(jnp.int32, (1, LAGS), 1) - LAGS // 2).astype(f32)
    col_w = jnp.sum(w, axis=0, keepdims=True)
    total = 1.0 + jnp.sum(col_w, axis=1, keepdims=True)
    row_m = jnp.sum(jnp.sum(w * da, axis=0, keepdims=True), axis=1, keepdims=True)
    col_m = jnp.sum(col_w * db, axis=1, keepdims=True)
    return p.astype(f32) + row_m / total, q.astype(f32) + col_m / total


def interleave(*works):
    for _ in zip(*works):
        pass


def make_kernel(sizes, rows_each):
    size_gz, size_row, size_col = sizes
    count = size_gz * size_row * size_col
    side = 2 * STRIDE
    margin = HALO // 2
    far = side - margin
    inner = far - margin
    mesh_id = pl.DeviceIdType.MESH
    cross = ((-1, 0), (1, 0), (0, -1), (0, 1))
    diagonal = ((-1, -1), (-1, 1), (1, -1), (1, 1))
    partners = sorted({1 % size_gz, size_gz - 1} - {0})
    reaches = doubling(sizes)
    rounds = len(reaches) + 2
    span = {-1: (0, margin), 0: (0, side), 1: (far, margin)}
    halo = {-1: (-margin, margin), 0: (0, side), 1: (side, margin)}
    chunks = (
        (0, margin, 0, margin), (0, margin, far, margin),
        (far, margin, 0, margin), (far, margin, far, margin),
        (margin, inner, 0, margin), (margin, inner, far, margin),
        (0, margin, margin, inner), (far, margin, margin, inner),
        (margin, inner, margin, inner),
    )
    copies = halo_copies(span, halo, margin, inner, cross, diagonal)

    def pick(section, *kinds):
        return [n for n, c in enumerate(copies) if c[0] == section and c[1] in kinds]

    def kernel(
        pri_hbm, order_hbm, sec_hbm, dft_hbm, wg_hbm, colc_hbm, cols_hbm, row_hbm, out_ref,
        ext, dft_ref, wg_ref, colc_ref, cols_ref, row_ref, first_ref, cross_ref, lags_ref, e_ref,
        pq_ref,
        mine_ref, all_ref,
        load_sem, halo_send, halo_recv, chunk_send, chunk_recv, flow_send, flow_recv, flood, pri_ref,
        order_ref,
    ):
        gz, row, col = lax.axis_index("gz"), lax.axis_index("row"), lax.axis_index("col")
        flat = (gz * size_row + row) * size_col + col

        def device(number):
            return (
                number // (size_row * size_col),
                (number // size_col) % size_row,
                number % size_col,
            )

        def exists(step):
            a, b = step
            ok = None
            for delta, place, size in ((a, row, size_row), (b, col, size_col)):
                if delta:
                    this = place > 0 if delta < 0 else place < size - 1
                    ok = this if ok is None else jnp.logical_and(ok, this)
            return ok

        near = len(partners)
        for step in cross:
            near = near + exists(step).astype(jnp.int32)

        def greet():
            barrier = pltpu.get_barrier_semaphore()
            for other in partners:
                pl.semaphore_signal(
                    barrier, 1, device_id=((gz + other) % size_gz, row, col),
                    device_id_type=mesh_id,
                )
            for step in cross:
                @pl.when(exists(step))
                def _(step=step):
                    pl.semaphore_signal(
                        barrier, 1, device_id=(gz, row + step[0], col + step[1]),
                        device_id_type=mesh_id,
                    )


        greet()
        loads = [
            pltpu.make_async_copy(
                sec_hbm.at[n], ext.at[n, margin : margin + side, margin : margin + side],
                load_sem.at[n],
            )
            for n in range(2)
        ]
        tables = (
            (dft_hbm, dft_ref), (wg_hbm, wg_ref), (row_hbm, row_ref), (pri_hbm, pri_ref),
            (order_hbm, order_ref), (colc_hbm, colc_ref), (cols_hbm, cols_ref),
        )
        for n, (source, target) in enumerate(tables):
            loads.append(pltpu.make_async_copy(source, target, load_sem.at[n + 2]))
        for copy in loads:
            copy.start()

        def place(section, r0, rn, c0, cn):
            return ext.at[
                section, margin + r0 : margin + r0 + rn, margin + c0 : margin + c0 + cn
            ]

        def landing(n):
            section, _, (a, b), _, (r0, rn, c0, cn) = copies[n]
            return place(section, r0 - a * side, rn, c0 - b * side, cn)

        def halo_copy(n):
            section, _, (a, b), _, box = copies[n]
            return pltpu.make_async_remote_copy(
                src_ref=place(section, *box), dst_ref=landing(n),
                send_sem=halo_send.at[n], recv_sem=halo_recv.at[n],
                device_id=(gz, row + a, col + b), device_id_type=mesh_id,
            )

        def guard(n, sign):
            _, kind, (a, b), side_col, _ = copies[n]
            if kind == "swing":
                return jnp.logical_and(row % 2 == 1, exists((1, sign * b)))
            ok = exists((sign * a, side_col if side_col else sign * b))
            if kind == "turn" and a < 0:
                ok = jnp.logical_and(ok, row % 2 == (1 if sign > 0 else 0))
            return ok

        def send(numbers):
            for n in numbers:
                @pl.when(guard(n, 1))
                def _(n=n):
                    halo_copy(n).start()

        def arrive(numbers):
            for n in numbers:
                @pl.when(guard(n, -1))
                def _(n=n):
                    ref = landing(n)
                    pltpu.make_async_copy(ref, ref, halo_recv.at[n]).wait()

        def chunk_copy(n):
            return pltpu.make_async_remote_copy(
                src_ref=place(0, *chunks[n]), dst_ref=place(2, *chunks[n]),
                send_sem=chunk_send.at[n], recv_sem=chunk_recv.at[n],
                device_id=((gz + size_gz - 1) % size_gz, row, col), device_id_type=mesh_id,
            )

        def took(low, high):
            for n in range(low, high):
                chunk_copy(n).wait_recv()

        def rung(n):
            if n < len(reaches):
                k = reaches[n]
                lines = []
                for way in (-k, k):
                    for axis, at, size in ((1, row, size_row), (2, col, size_col)):
                        ok = at + way >= 0 if way < 0 else at + way < size
                        lines.append((ok, (gz, row + way, col) if axis == 1 else (gz, row, col + way)))
                return lines
            if n == len(reaches):
                return [(None, (gz, row, (col + j) % size_col)) for j in range(1, size_col)]
            return [(None, ((gz + j) % size_gz, row, col)) for j in range(1, size_gz)]

        def climb(n):
            for ok, target in rung(n):
                def tell(target=target):
                    pl.semaphore_signal(
                        flood.at[n], 1, device_id=target, device_id_type=mesh_id
                    )
                if ok is None:
                    tell()
                else:
                    pl.when(ok)(tell)

        def heard(n):
            total = 0
            for ok, _ in rung(n):
                total = total + (1 if ok is None else ok.astype(jnp.int32))
            return total

        done = [0]

        def spread(upto):
            for n in range(done[0], min(upto, rounds)):
                pl.semaphore_wait(flood.at[n], heard(n))
                if n + 1 < rounds:
                    climb(n + 1)
            done[0] = max(done[0], min(upto, rounds))

        wide = ext.shape[2]
        edge, last = margin, wide - margin
        spans_of = {
            "middle": ((edge, last),),
            "outer": ((0, edge), (last, wide)),
            "sides": ((0, 2 * edge), (last - edge, wide)),
            "center": ((2 * edge, last - edge),),
        }

        def columns_pass(section, part):
            first_pass(ext, section, dft_ref, pq_ref, 2 * (section % 2), spans_of[part])

        lane = lax.broadcasted_iota(jnp.int32, (1, LAGS), 1)
        sections, columns = 2 * size_gz, 2 * size_col

        def prior(part, section, i, j):
            return pri_ref[part, section, i, j]

        def patch(section, i, j):
            return spectrum_work(
                wg_ref, pq_ref, 2 * (section % 2) + i, j, first_ref, 2 * i + j,
                cross_ref if section else None, section < 2,
            )

        def flows(section, surfaces):
            values = []
            for n in range(4):
                p, q = prior(0, section - 1, n // 2, n % 2), prior(1, section - 1, n // 2, n % 2)
                a, b = centroid(surfaces[n], p, q)
                at = (2 * gz + section - 1) * columns + 2 * col + n % 2
                value = jnp.where(lane == at, a, 0.0)
                values.append(value + jnp.where(lane == at + sections * columns, b, 0.0))
            mine_ref[0] = mine_ref[0] + values[0] + values[1]
            mine_ref[1] = mine_ref[1] + values[2] + values[3]

        def patches(section, event=None):
            halves, surfaces = {}, {}

            def spectra(i):
                return [patch(section, i, j) for j in range(2)]

            def half(i):
                return [
                    half_work(cross_ref, n, e_ref, 4 * (section - 1) + n, halves)
                    for n in (2 * i, 2 * i + 1)
                ]

            def surface(i):
                for n in (2 * i, 2 * i + 1):
                    surfaces[n] = surface_of(halves[n], lags_ref[4 * (section - 1) + n])

            interleave(*spectra(0))
            if not section:
                interleave(*spectra(1))
                return
            if event is not None:
                event()
            interleave(*half(0), *spectra(1))
            interleave(*half(1))
            surface(0)
            surface(1)
            flows(section, surfaces)

        def lag_prepare(n, carry):
            lags_ref[n] = lag_rows(row_ref, prior(0, n // 4, (n // 2) % 2, n % 2))
            shift = prior(1, n // 4, (n // 2) % 2, n % 2) + LAGS // 2
            for g in range(4):
                ec = colc_ref[g, pl.ds(shift, LAGS), :]
                es = cols_ref[g, pl.ds(shift, LAGS), :]
                tiles = ((ec, -es), (es, ec))
                for a in range(2):
                    for b in range(2):
                        at = (2 * g + b) * QUARTER
                        e_ref[n, a * LAGS : (a + 1) * LAGS, at : at + QUARTER] = tiles[a][b].astype(
                            jnp.bfloat16
                        )
            return carry

        for step in cross + diagonal:
            @pl.when(jnp.logical_not(exists(step)))
            def _(step=step):
                (r0, rn), (c0, cn) = halo[step[0]], halo[step[1]]
                ext[:, margin + r0 : margin + r0 + rn, margin + c0 : margin + c0 + cn] = (
                    jnp.zeros((3, rn, cn), ext.dtype)
                )

        mine_ref[...] = jnp.zeros_like(mine_ref)
        pl.semaphore_wait(pltpu.get_barrier_semaphore(), near)
        loads[0].wait()
        for n in range(len(chunks)):
            chunk_copy(n).start()
        send(pick(0, "row", "col"))
        loads[1].wait()
        send(pick(1, "row", "col"))
        climb(0)
        for copy in loads[2:]:
            copy.wait()

        def top():
            took(6, 7)
            send(pick(2, "up"))

        def bottom():
            took(7, 8)
            send(pick(2, "down"))

        lax.fori_loop(0, 8, lag_prepare, 0)
        arrive(pick(0, "row"))
        send(pick(0, "swing"))
        columns_pass(0, "middle")
        spread(1)
        arrive(pick(0, "col"))
        send(pick(0, "turn"))
        arrive(pick(1, "row"))
        send(pick(1, "swing"))
        took(0, 4)
        send(pick(2, "diagonal", "corner"))
        columns_pass(1, "middle")
        spread(2)
        took(4, 5)
        send(pick(2, "left"))
        arrive(pick(1, "col"))
        send(pick(1, "turn"))
        took(5, 6)
        send(pick(2, "right"))
        arrive(pick(0, "turn", "swing"))
        columns_pass(0, "outer")
        patches(0)
        spread(3)
        top()
        pl.when(row % 2 == 1)(bottom)
        arrive(pick(1, "turn", "swing"))
        columns_pass(1, "outer")
        patches(1)
        pl.when(row % 2 == 0)(bottom)
        arrive(pick(2, "left", "right", "diagonal", "corner"))
        columns_pass(2, "sides")
        took(8, 9)
        arrive(pick(2, "up", "down"))
        columns_pass(2, "center")
        patches(2)
        spread(rounds)

        total_rows = 2 * size_row
        slot = gz * size_col + col
        spot = slot * total_rows + 2 * row

        rows_on = [(row + n) % size_row for n in range(size_row)]
        cols_on = [(col + n) % size_col for n in range(size_col)]
        for a in range(size_gz):
            plane = (gz + a) % size_gz
            for b in range(size_row):
                for c in range(size_col):
                    if a + b + c:
                        pltpu.make_async_remote_copy(
                            src_ref=mine_ref, dst_ref=all_ref.at[pl.ds(spot, 2)],
                            send_sem=flow_send, recv_sem=flow_recv,
                            device_id=(plane, rows_on[b], cols_on[c]), device_id_type=mesh_id,
                        ).start()
        all_ref[spot] = mine_ref[0]
        all_ref[spot + 1] = mine_ref[1]
        for n in range(len(chunks)):
            chunk_copy(n).wait_send()
        for n in range(len(copies)):
            @pl.when(guard(n, 1))
            def _(n=n):
                halo_copy(n).wait_send()
        got = all_ref.at[pl.ds(0, 2 * (count - 1))]
        pltpu.make_async_copy(got, got, flow_recv).wait()
        for m in range(rows_each):
            wanted = order_ref[row * rows_each + m]
            value = all_ref[wanted]
            for other in range(1, size_gz * size_col):
                value = value + all_ref[other * total_rows + wanted]
            out_ref[m : m + 1, :] = value[:, : out_ref.shape[1]]
        pltpu.make_async_copy(got, got, flow_send).wait()

    return kernel


def doubling(sizes):
    reaches = [1]
    while 2 * reaches[-1] < max(sizes[1:]):
        reaches.append(2 * reaches[-1])
    return reaches


def halo_copies(span, halo, margin, inner, cross, diagonal):
    copies = []
    for section in range(2):
        for step in cross:
            kind = "row" if step[0] else "col"
            copies.append((section, kind, step, 0, span[step[0]] + span[step[1]]))
        for a, b in diagonal:
            copies.append((section, "turn", (a, 0), b, span[a] + halo[b]))
        for b in (-1, 1):
            copies.append((section, "swing", (0, b), 0, halo[1] + span[b]))
    for a, b in diagonal:
        copies.append((2, "diagonal", (a, b), 0, span[a] + span[b]))
    for a, b in diagonal:
        copies.append((2, "corner", (a, 0), 0, span[a] + span[b]))
    for b in (-1, 1):
        copies.append((2, "left" if b < 0 else "right", (0, b), 0, span[0] + span[b]))
    for a in (-1, 1):
        copies.append((2, "up" if a < 0 else "down", (a, 0), 0, span[a] + (margin, inner)))
    return copies


def body(sections, priors, row_order):
    sizes = tuple(lax.axis_size(name) for name in ("gz", "row", "col"))
    count = math.prod(sizes)
    rows_each = row_order.shape[0] // sizes[1]
    width = 2 * 2 * sizes[0] * 2 * sizes[2]
    colc, cols = column_tables()
    tables = (
        bf16_const(dft_table()),
        bf16_const(split_tables()),
        f32_const(lane_tiles(colc)),
        f32_const(lane_tiles(cols)),
        f32_const(lane_tiles(lag_table())),
    )
    hbm = pl.BlockSpec(memory_space=pl.ANY)
    dma = pltpu.SemaphoreType.DMA
    wide = 2 * STRIDE + HALO
    flows = pl.pallas_call(
        make_kernel(sizes, rows_each),
        out_shape=jax.ShapeDtypeStruct((rows_each, width), jnp.float32),
        in_specs=[hbm] * 8,
        out_specs=pl.BlockSpec(memory_space=pltpu.VMEM),
        scratch_shapes=[
            pltpu.VMEM((3, wide, wide), jnp.bfloat16),
            *[pltpu.VMEM(t.shape, t.dtype) for t in tables],
            pltpu.VMEM((4, KROWS, 2 * PATCH), jnp.float32),
            pltpu.VMEM((4, KROWS, 2 * PATCH), jnp.bfloat16),
            pltpu.VMEM((8, LAGS, PATCH), jnp.bfloat16),
            pltpu.VMEM((8, 2 * LAGS, 2 * PATCH), jnp.bfloat16),
            pltpu.VMEM((4, 2 * KROWS, wide), jnp.float32),
            pltpu.VMEM((2, 1, LAGS), jnp.float32),
            pltpu.VMEM((2 * count, 1, LAGS), jnp.float32),
            dma((9,)), dma((32,)), dma((32,)), dma((9,)), dma((9,)), dma(()), dma(()),
            pltpu.SemaphoreType.REGULAR((len(doubling(sizes)) + 2,)),
            pltpu.SMEM(priors.shape, priors.dtype), pltpu.SMEM(row_order.shape, row_order.dtype),
        ],
        compiler_params=pltpu.CompilerParams(
            vmem_limit_bytes=41943040, collective_id=0, has_side_effects=True,
        ),
    )(*[pltpu.with_memory_space_constraint(x, pltpu.HBM) for x in (priors, row_order, sections, *tables)])
    return flows


def solution(mesh):
    placed = (P("gz", "row", "col"), P(None, "gz", "row", "col"), P())
    return jax.shard_map(
        body, mesh=mesh, in_specs=placed, out_specs=P("row", None), check_vma=False
    )
```
